32 devices in a mesh: grp: 2 (over y), lon: 4 (over z), lat: 2 (over x), lvl: 2 (over core).
Axes of the slice: x: 2, y: 2, z: 4, core: 2. Of those that a mesh axis runs over, the one named last changes fastest.
Arguments:
- tokens: bfloat16 [4, 24, 96, 512], P(('grp', 'lvl'), 'lat', 'lon'), parts along dimension 0, may hold values from -8 to 8
- fine_tags: int32 [4, 24, 96], P(('grp', 'lvl'), 'lat', 'lon'), parts along dimension 0, may hold values from 1 to 3
- coarse_tags: int32 [4, 12, 48], P(('grp', 'lvl'), 'lat', 'lon'), parts along dimension 0, may hold values from 1 to 3
- fine_gain: float32 [512], replicated, may hold values from 0.25 to 1.75
- fine_inward: bfloat16 [3, 512, 512], P(None, 'lon', 'lvl'), may hold values from -0.25 to 0.25
- fine_outward: bfloat16 [512, 512], P('lon', 'lvl'), may hold values from -0.25 to 0.25
- fine_table: float32 [16, 253], replicated, may hold values from -2 to 300
- merge_gain: float32 [2048], replicated, may hold values from 0.25 to 1.75
- merge_weight: bfloat16 [1024, 2048], P('lon', 'lvl'), may hold values from -0.125 to 0.125
- coarse_gain: float32 [1024], replicated, may hold values from 0.25 to 1.75
- coarse_inward: bfloat16 [3, 1024, 1024], P(None, 'lon', 'lvl'), may hold values from -0.1875 to 0.1875
- coarse_outward: bfloat16 [1024, 1024], P('lon', 'lvl'), may hold values from -0.1875 to 0.1875
- coarse_table: float32 [32, 253], replicated, may hold values from -2 to 300
Outputs:
- fine_out: bfloat16 [4, 24, 96, 512], P(('grp', 'lvl'), 'lat', 'lon'), parts along dimension 0
- coarse_out: bfloat16 [4, 12, 48, 1024], P(('grp', 'lvl'), 'lat', 'lon'), parts along dimension 0
The draws below stay inside these ranges and needn't reach their ends.
There are 2 independent parts, one for each index of `grp`. The reference program is written for one: setup_inputs(seed, part) draws one part's arguments, and reference() takes and returns one part's arrays. A program takes and returns all parts, laid end to end along the dimension named above; an argument that names none is the same for every part. Nothing has to cross between parts.
All inputs are finite; a program needn't handle non-finite values.
Results may differ from the reference program's by a relative error of at most 0.017.
Values may be sent and summed in bfloat16 or wider, within the bound.
A program may use at most 64 MiB of HBM per device.

```python
import jax
import jax.numpy as jnp
from jax import lax

D1 = 512
HEADS1 = 16
D2 = 1024
HEADS2 = 32
WIN_LAT = 6
WIN_LON = 12
LEVELS = 2
LATS = 24
LONS = 96


def draw_tokens(key, part):
    normal_key = jax.random.fold_in(key, 0)
    sample = jax.random.normal(normal_key, (LEVELS, LATS, LONS, D1), jnp.float32)
    return jnp.clip(sample, -8.0, 8.0).astype(jnp.float32).astype(jnp.bfloat16)


def table_draw(seed_key, head_count):
    base_key = jax.random.fold_in(seed_key, 0)
    span_lat = 2 * WIN_LAT - 1
    span_lon = 2 * WIN_LON - 1
    baseline = jax.random.uniform(base_key, (head_count, span_lat * span_lon), jnp.float32, -2.0, 2.0)
    return baseline


def draw_fine_table(key, part):
    return table_draw(jax.random.fold_in(key, 11), HEADS1)


def draw_coarse_table(key, part):
    return table_draw(jax.random.fold_in(key, 23), HEADS2)


def with_ends(entries, stream_key, smallest, high):
    longest = entries.shape.index(max(entries.shape))
    spots = []
    for shift in (0, 1):
        where = [jax.random.randint(jax.random.fold_in(stream_key, axis), (), 0, length) for axis, length in enumerate(entries.shape)]
        where[longest] = (where[longest] + shift) % entries.shape[longest]
        spots.append(tuple(where))
    return entries.at[spots[0]].set(smallest).at[spots[1]].set(high)


def level_of(own_key, extent, pieces, least, largest):
    factor_of, own = 1.0, jax.random.fold_in(own_key, 6)
    for position, blocks in pieces:
        steps = jnp.exp(jax.random.uniform(jax.random.fold_in(own, position), (blocks,), jnp.float32, least / len(pieces), largest / len(pieces)))
        factor_of = factor_of * jnp.repeat(steps, extent[position] // blocks).reshape([-1 if axis == position else 1 for axis in range(len(extent))])
    return factor_of


def gaussian(own_key, dims, width, limit, cuts=(), kind=jnp.bfloat16):
    array = width * jax.random.normal(own_key, dims, jnp.float32)
    if cuts:
        array = array * level_of(own_key, dims, cuts, -0.22, 0.18)
    return jnp.clip(array, -limit, limit).astype(kind)


def setup_inputs(seed: int = 0, part: int = 0) -> dict:
    splits = jax.random.split(jax.random.key(seed), 14)
    part_keys = jax.random.split(jax.random.fold_in(splits[13], part), 14)
    tokens = draw_tokens(jax.random.fold_in(jax.random.fold_in(splits[13], part), 71), part)
    fine_tags = with_ends(jax.random.randint(part_keys[1], (LEVELS, LATS, LONS), 1, 4), jax.random.fold_in(part_keys[1], 1), 1, 3).astype(jnp.int32)
    coarse_tags = with_ends(jax.random.randint(part_keys[2], (LEVELS, LATS // 2, LONS // 2), 1, 4), jax.random.fold_in(part_keys[2], 1), 1, 3).astype(jnp.int32)
    fine_gain = jnp.clip(1.0 + 0.15 * jax.random.normal(splits[3], (D1,), jnp.float32), 0.25, 1.75)
    fine_inward = gaussian(splits[4], (3, D1, D1), D1 ** -0.5, 0.25, ((1, 4), (2, 2)))
    fine_outward = gaussian(splits[5], (D1, D1), D1 ** -0.5, 0.25, ((0, 4), (1, 2)))
    fine_table = draw_fine_table(jax.random.fold_in(splits[13], 71), part)
    merge_gain = jnp.clip(1.0 + 0.15 * jax.random.normal(splits[7], (4 * D1,), jnp.float32), 0.25, 1.75)
    merge_weight = gaussian(splits[8], (D2, 4 * D1), (4 * D1) ** -0.5, 0.125, ((0, 4), (1, 2)))
    coarse_gain = jnp.clip(1.0 + 0.15 * jax.random.normal(splits[9], (D2,), jnp.float32), 0.25, 1.75)
    coarse_inward = gaussian(splits[10], (3, D2, D2), D2 ** -0.5, 0.1875, ((1, 4), (2, 2)))
    coarse_outward = gaussian(splits[11], (D2, D2), D2 ** -0.5, 0.1875, ((0, 4), (1, 2)))
    coarse_table = draw_coarse_table(jax.random.fold_in(splits[13], 71), part)
    return dict(tokens=tokens, fine_tags=fine_tags, coarse_tags=coarse_tags, fine_gain=fine_gain, fine_inward=fine_inward, fine_outward=fine_outward, fine_table=fine_table, merge_gain=merge_gain, merge_weight=merge_weight, coarse_gain=coarse_gain, coarse_inward=coarse_inward, coarse_outward=coarse_outward, coarse_table=coarse_table)


EPSILON = 1e-05

def layer_norm(values, scales):
    widened = values.astype(jnp.float32)
    center = widened - lax.optimization_barrier(jnp.mean(widened, axis=-1, keepdims=True))
    spread = lax.optimization_barrier(jnp.mean(center * center, axis=-1, keepdims=True))
    return center * lax.rsqrt(spread + EPSILON) * scales.astype(jnp.float32)

def bias_blocks(bias_table, win_lat, win_lon):
    head_count = bias_table.shape[0]
    span_lat = 2 * win_lat - 1
    span_lon = 2 * win_lon - 1
    table_grid = bias_table.astype(jnp.float32).reshape(head_count, span_lat, span_lon)
    lat_pos = jnp.arange(win_lat)
    lon_pos = jnp.arange(win_lon)
    lat_onehot = (lat_pos[:, None, None] - lat_pos[None, :, None] + win_lat - 1 == jnp.arange(span_lat)[None, None, :]).astype(jnp.float32)
    lon_onehot = (lon_pos[:, None, None] - lon_pos[None, :, None] + win_lon - 1 == jnp.arange(span_lon)[None, None, :]).astype(jnp.float32)
    along_lon = jnp.einsum('hab,ijb->haij', table_grid, lon_onehot, precision=lax.Precision.HIGHEST)
    blocks = jnp.einsum('kla,haij->hkilj', lat_onehot, along_lon, precision=lax.Precision.HIGHEST)
    return blocks.reshape(head_count, win_lat * win_lon, win_lat * win_lon)

def split_windows(array_in, win_lat, win_lon):
    levels, lat_len, lon_len = array_in.shape[:3]
    trailing = array_in.shape[3:]
    blocked = array_in.reshape((levels, lat_len // win_lat, win_lat, lon_len // win_lon, win_lon) + trailing)
    blocked = jnp.moveaxis(blocked, 3, 2)
    return blocked.reshape((levels, lat_len // win_lat, lon_len // win_lon, win_lat * win_lon) + trailing)

def join_windows(array_in, win_lat, win_lon):
    levels, lat_bands, lon_bands = array_in.shape[:3]
    trailing = array_in.shape[4:]
    blocked = array_in.reshape((levels, lat_bands, lon_bands, win_lat, win_lon) + trailing)
    blocked = jnp.moveaxis(blocked, 3, 2)
    return blocked.reshape((levels, lat_bands * win_lat, lon_bands * win_lon) + trailing)

def attend(query_grid, key_grid, value_grid, tag_grid, bias_table, win_lat, win_lon):
    head_count = bias_table.shape[0]
    features = query_grid.shape[-1]
    head_size = features // head_count
    offsets_bias = bias_blocks(bias_table, win_lat, win_lon)

    def heads_of(array_in):
        blocks = split_windows(array_in, win_lat, win_lon)
        return blocks.reshape((-1,) + blocks.shape[2:4] + (head_count, head_size)).astype(jnp.float32)
    query_heads = heads_of(query_grid)
    key_heads = heads_of(key_grid)
    value_heads = heads_of(value_grid)
    tag_blocks = split_windows(tag_grid, win_lat, win_lon)
    tag_blocks = tag_blocks.reshape((-1,) + tag_blocks.shape[2:4])

    def one_band(inputs):
        query_band, key_band, value_band, tag_band = inputs
        scores = jnp.einsum('bphd,bqhd->bhpq', query_band, key_band, precision=lax.Precision.HIGHEST)
        scores = scores * head_size ** (-0.5) + offsets_bias
        allowed = tag_band[:, None, :, None] == tag_band[:, None, None, :]
        scores = jnp.where(allowed, scores, -jnp.inf)
        highest = lax.optimization_barrier(jnp.max(scores, axis=-1, keepdims=True))
        weights = jnp.exp(scores - highest)
        shares = (weights / lax.optimization_barrier(jnp.sum(weights, axis=-1, keepdims=True))).astype(jnp.bfloat16)
        blended = jnp.einsum('bhpq,bqhd->bphd', shares.astype(jnp.float32), value_band, precision=lax.Precision.HIGHEST)
        return blended.astype(jnp.bfloat16).reshape(blended.shape[:2] + (features,))
    blended = lax.map(one_band, (query_heads, key_heads, value_heads, tag_blocks))
    levels, lat_len = query_grid.shape[:2]
    blended = blended.reshape((levels, lat_len // win_lat) + blended.shape[1:])
    return join_windows(blended, win_lat, win_lon)

def window_block(stream, tag_grid, gain_row, inward, outward, bias_table):
    levels, lat_len, lon_len, features = stream.shape
    normed = layer_norm(stream, gain_row).astype(jnp.bfloat16)
    flattened = normed.reshape(-1, features)
    lat_half = WIN_LAT // 2
    lon_half = WIN_LON // 2

    def arrange(array_in):
        rolled = jnp.roll(array_in, -lon_half, axis=2)
        padding = [(0, 0), (lat_half, lat_half)] + [(0, 0)] * (array_in.ndim - 2)
        return jnp.pad(rolled, padding)
    projected = []
    for member in range(3):
        product = jnp.dot(flattened, inward[member], preferred_element_type=jnp.float32).astype(jnp.bfloat16)
        projected.append(arrange(product.reshape(levels, lat_len, lon_len, features)))
    blended = attend(projected[0], projected[1], projected[2], arrange(tag_grid), bias_table, WIN_LAT, WIN_LON)
    blended = jnp.roll(blended[:, lat_half:lat_half + lat_len], lon_half, axis=2)
    update = jnp.dot(blended.reshape(-1, features), outward.T, preferred_element_type=jnp.float32)
    return (stream.astype(jnp.float32) + update.reshape(stream.shape)).astype(jnp.bfloat16)

def group_patches(stream):
    levels, lat_len, lon_len, features = stream.shape
    blocked = stream.reshape(levels, lat_len // 2, 2, lon_len // 2, 2, features)
    blocked = jnp.moveaxis(blocked, 3, 2)
    return blocked.reshape(levels, lat_len // 2, lon_len // 2, 4 * features)

def reference(tokens, fine_tags, coarse_tags, fine_gain, fine_inward, fine_outward, fine_table, merge_gain, merge_weight, coarse_gain, coarse_inward, coarse_outward, coarse_table):
    fine_result = window_block(tokens, fine_tags, fine_gain, fine_inward, fine_outward, fine_table)
    grouped = group_patches(fine_result)
    merged_normed = layer_norm(grouped, merge_gain).astype(jnp.bfloat16)
    levels, lat_len, lon_len, wide_features = merged_normed.shape
    coarse_in = jnp.dot(merged_normed.reshape(-1, wide_features), merge_weight.T, preferred_element_type=jnp.float32)
    coarse_in = coarse_in.astype(jnp.bfloat16).reshape(levels, lat_len, lon_len, -1)
    coarse_result = window_block(coarse_in, coarse_tags, coarse_gain, coarse_inward, coarse_outward, coarse_table)
    return (fine_result, coarse_result)
```

```python
import functools
import math

import jax
import jax.numpy as jnp
import numpy as np
from jax import lax
from jax.experimental import pallas as pl
from jax.experimental.pallas import tpu as pltpu
from jax.sharding import PartitionSpec as P

WIN_LAT = 6
WIN_LON = 12
HALF_LAT = WIN_LAT // 2
HALF_LON = WIN_LON // 2
QUAD = HALF_LAT * HALF_LON
ROWS = -(-QUAD // 16) * 16
WINDOW = 4 * ROWS
EPSILON = 1e-05
LANES = 128
LOG2E = math.log2(math.e)
MESH = pl.DeviceIdType.MESH
VMEM = pl.BlockSpec(memory_space=pltpu.VMEM)
ANY = pl.BlockSpec(memory_space=pl.ANY)
LIMIT = 60 * 1024 * 1024
NT = (((1,), (1,)), ((), ()))
AROUND = ((0, -1), (0, 1), (-1, 0), (1, 0), (-1, -1), (-1, 1), (1, -1), (1, 1))
AHEAD = 2


def up_to(count, step):
    return -(-count // step) * step


class Plan:
    def __init__(self, lat_len, lon_len):
        self.lat_len, self.lon_len = lat_len, lon_len
        self.own = lat_len * lon_len
        self.down, self.across = lat_len // HALF_LAT, lon_len // HALF_LON
        self.quads = self.down * self.across
        self.columns = self.across // 2 + 1
        self.windows = (self.down // 2 + 1) * self.columns
        self.halo = []
        for side, (dy, dx) in enumerate(AROUND):
            rows = [-1] if dy < 0 else ([self.down] if dy > 0 else range(self.down))
            cols = [-1] if dx < 0 else ([self.across] if dx > 0 else range(self.across))
            for r in rows:
                for c in cols:
                    self.halo.append((side, r, c, (r % self.down) * self.across + c % self.across))

    def spot(self, r, c):
        window = ((r + 1) // 2) * self.columns + (c + 1) // 2
        return 4 * window + ((r + 1) % 2) * 2 + (c + 1) % 2

    def natural(self):
        result = np.full((self.quads * ROWS,), -1, np.int32)
        for q in range(self.quads):
            for p in range(QUAD):
                r = (q // self.across) * HALF_LAT + p // HALF_LON
                c = (q % self.across) * HALF_LON + p % HALF_LON
                result[q * ROWS + p] = r * self.lon_len + c
        return result

    def back(self, pitch):
        result = np.full((self.lat_len * pitch,), -1, np.int32)
        for row, token in enumerate(self.natural()):
            if token >= 0:
                result[token // self.lon_len * pitch + token % self.lon_len] = row
        return result

    def lanes(self):
        lane = np.arange(self.across * LANES)
        place = lane % ROWS
        column = (lane // LANES) * HALF_LON + place % HALF_LON
        return np.where(place < QUAD, column, -1), np.where(place < QUAD, place // HALF_LON, -1)


def patches(fine, coarse):
    token = coarse.natural()
    result = []
    for s in range(2):
        for t in range(2):
            a, b = token // coarse.lon_len, token % coarse.lon_len
            result.append(np.where(token >= 0, (2 * a + s) * fine.lon_len + 2 * b + t, -1))
    return np.concatenate(result)


def offset_numbers():
    spot = np.arange(WINDOW)
    place = spot % ROWS
    r = spot // ROWS // 2 * HALF_LAT + place // HALF_LON
    c = spot // ROWS % 2 * HALF_LON + place % HALF_LON
    number = (r[:, None] - r[None, :] + WIN_LAT - 1) * (2 * WIN_LON - 1) + c[:, None] - c[None, :] + WIN_LON - 1
    valid = (place < QUAD)[:, None] & (place < QUAD)[None, :]
    return np.where(valid, number, -1).astype(np.int32)


def onehot(index, width):
    spots = lax.broadcasted_iota(jnp.int32, (index.shape[0], width), 1)
    return jnp.where(spots == index, 1.0, 0.0).astype(jnp.bfloat16)


def pick(index, source):
    return jnp.dot(
        onehot(index, source.shape[0]), source, preferred_element_type=jnp.float32
    ).astype(jnp.bfloat16)


def normalize(values, gain):
    widened = values.astype(jnp.float32)
    center = widened - jnp.mean(widened, axis=-1, keepdims=True)
    spread = jnp.mean(center * center, axis=-1, keepdims=True)
    return (center * lax.rsqrt(spread + EPSILON) * gain).astype(jnp.bfloat16)


class Around:
    def __init__(self):
        self.lat, self.lon = lax.axis_index("lat"), lax.axis_index("lon")
        self.lats, self.lons = lax.axis_size("lat"), lax.axis_size("lon")

    def place(self, dy, dx):
        return {
            "lat": lax.rem(self.lat + dy + self.lats, self.lats),
            "lon": lax.rem(self.lon + dx + self.lons, self.lons),
        }

    def there(self, dy):
        return (self.lat > 0) if dy < 0 else (self.lat < self.lats - 1)

    def when_there(self, dy, action):
        if dy == 0:
            action()
        else:
            pl.when(self.there(dy))(action)

    def greet(self, barrier):
        for dy, dx in AROUND:
            def signal(dy=dy, dx=dx):
                pl.semaphore_signal(barrier, inc=1, device_id=self.place(dy, dx), device_id_type=MESH)
            self.when_there(dy, signal)
        return 2 + 3 * (self.lat > 0).astype(jnp.int32) + 3 * (self.lat < self.lats - 1).astype(jnp.int32)

    def copy(self, src, dst, send, recv, dy, dx):
        return pltpu.make_async_remote_copy(
            src_ref=src, dst_ref=dst, send_sem=send, recv_sem=recv,
            device_id=self.place(-dy, -dx), device_id_type=MESH,
        )


class Halo:
    def __init__(self, around, plan, own, wide, send, recv):
        self.around, self.plan, self.own, self.wide, self.send, self.recv = around, plan, own, wide, send, recv

    def copy(self, n):
        side, r, c, q = self.plan.halo[n]
        return self.around.copy(
            self.own.at[pl.ds(q * ROWS, ROWS)], self.wide.at[pl.ds(self.plan.spot(r, c) * ROWS, ROWS)],
            self.send.at[n], self.recv.at[n], *AROUND[side],
        )

    def start(self):
        for n, (side, r, c, _) in enumerate(self.plan.halo):
            dy = AROUND[side][0]
            self.around.when_there(-dy, lambda n=n: self.copy(n).start())
            if dy:
                def clear(r=r, c=c):
                    rows = pl.ds(self.plan.spot(r, c) * ROWS, ROWS)
                    self.wide[rows, :] = jnp.zeros((ROWS, self.wide.shape[1]), self.wide.dtype)
                pl.when(jnp.logical_not(self.around.there(dy)))(clear)

    def finish(self):
        for n, (side, *_) in enumerate(self.plan.halo):
            self.around.when_there(AROUND[side][0], lambda n=n: self.copy(n).wait_recv())

    def drain(self):
        for n, (side, *_) in enumerate(self.plan.halo):
            self.around.when_there(-AROUND[side][0], lambda n=n: self.copy(n).wait_send())


class Gather:
    def __init__(self, shards, fulls, units, split, sems):
        self.shards, self.fulls, self.units, self.split, self.sems = shards, fulls, units, split, sems
        self.index = {a: lax.axis_index(a) for a in ("grp", "lat", "lon", "lvl")}
        self.size = {a: lax.axis_size(a) for a in ("grp", "lat", "lon", "lvl")}
        self.halves = range(2 if split else 1)
        self.ways = [(s, half) for s in range(1, self.size["lon"]) for half in self.halves]
        self.now = 0
        self.steps = len(units) + (2 if split else 0)

    def at(self, axis, step):
        return {axis: lax.rem(self.index[axis] + step + self.size[axis], self.size[axis])}

    def greet(self, barrier):
        peers = 0
        for axis in ("lon", "lvl", "lat", "grp") if self.split else ("lon", "lvl"):
            for d in range(1, self.size[axis]):
                pl.semaphore_signal(barrier, inc=1, device_id=self.at(axis, d), device_id_type=MESH)
                peers += 1
        return peers

    def block_of(self, slot):
        return lax.rem(self.index["lon"] + slot, self.size["lon"]) if self.split else slot

    def rows(self, u):
        return self.shards[self.units[u][0]].shape[1]

    def axes(self, half):
        return ("lat", "grp") if half == 0 else ("grp", "lat")

    def piece(self, u, half):
        if not self.split:
            return 0, self.rows(u)
        size = self.rows(u) // 8
        first, second = self.axes(half)
        order = self.index[second] * 2 + self.index[first]
        return pl.multiple_of((half * 4 + order) * size, 16), size

    def pair(self, u, half):
        size = self.rows(u) // 8
        return pl.multiple_of((half * 4 + self.index[self.axes(half)[1]] * 2) * size, 16), 2 * size

    def held(self, u, start, size):
        m, k, depth, col, cols = self.units[u]
        return self.shards[m].at[pl.ds(k, depth), pl.ds(start, size), pl.ds(col, cols)]

    def block(self, u, slot, slots, start, size):
        m, k, depth, col, cols = self.units[u]
        return self.fulls[m].at[
            self.index["lvl"], pl.ds(k, depth), pl.ds(slot, slots), pl.ds(start, size), pl.ds(col, cols)
        ]

    def slot(self, u, slot, start, size):
        m, k, depth, col, cols = self.units[u]
        return self.fulls[m].at[self.index["lvl"], pl.ds(k, depth), slot, pl.ds(start, size), pl.ds(col, cols)]

    def remote(self, src, dst, kind, number, device):
        send, recv = self.sems[1 + 2 * kind], self.sems[2 + 2 * kind]
        return pltpu.make_async_remote_copy(
            src_ref=src, dst_ref=dst, send_sem=send.at[number], recv_sem=recv.at[number],
            device_id=device, device_id_type=MESH,
        )

    def own_copy(self, u):
        slot = 0 if self.split else self.index["lon"]
        return pltpu.make_async_copy(
            self.held(u, 0, self.rows(u)), self.slot(u, slot, 0, self.rows(u)), self.sems[0].at[u]
        )

    def lon_copy(self, u, s, half):
        start, size = self.piece(u, half)
        slot = s if self.split else self.index["lon"]
        return self.remote(
            self.held(u, start, size), self.slot(u, slot, start, size), 0, (u, s - 1, half), self.at("lon", -s)
        )

    def one_copy(self, u, half):
        block = self.block(u, 1, self.size["lon"] - 1, *self.piece(u, half))
        return self.remote(block, block, 1, (u, half), self.at(self.axes(half)[0], 1))

    def two_copy(self, u, half):
        block = self.block(u, 1, self.size["lon"] - 1, *self.pair(u, half))
        return self.remote(block, block, 2, (u, half), self.at(self.axes(half)[1], 1))

    def lvl_copy(self, u):
        block = self.block(u, 0, self.size["lon"], 0, self.rows(u))
        return self.remote(block, block, 3, (u,), self.at("lvl", 1))

    def issue(self, u):
        if u < len(self.units):
            for s, half in self.ways:
                self.lon_copy(u, s, half).start()
            self.own_copy(u).start()

    def begin(self):
        for u in range(AHEAD):
            self.issue(u)

    def step(self):
        k, count = self.now, len(self.units)
        self.now += 1
        if k < count:
            for half in self.halves:
                for s in range(1, self.size["lon"]):
                    self.lon_copy(k, s, half).wait_recv()
                if self.split:
                    self.one_copy(k, half).start()
            self.issue(k + AHEAD)
        if self.split and 0 <= k - 1 < count:
            for half in self.halves:
                self.one_copy(k - 1, half).wait_recv()
                self.two_copy(k - 1, half).start()
        done = k - 2 if self.split else k
        if 0 <= done < count:
            if self.split:
                for half in self.halves:
                    self.two_copy(done, half).wait_recv()
            self.own_copy(done).wait()
            self.lvl_copy(done).start()

    def ready(self, *wanted):
        for u in wanted:
            while self.now <= u + (2 if self.split else 0):
                self.step()
            self.lvl_copy(u).wait_recv()

    def end(self):
        for u in range(len(self.units)):
            self.lvl_copy(u).wait_send()
            for s, half in self.ways:
                self.lon_copy(u, s, half).wait_send()
            if self.split:
                for half in self.halves:
                    self.one_copy(u, half).wait_send()
                    self.two_copy(u, half).wait_send()


def weight_units(shards):
    fine_inward, fine_outward, merge, coarse_inward, coarse_outward = [s.shape for s in shards]
    units = [(0, k, 1, 0, fine_inward[2]) for k in range(3)]
    units.append((1, 0, 1, 0, fine_outward[2]))
    units += [(2, 0, 1, c, merge[2] // 4) for c in range(0, merge[2], merge[2] // 4)]
    units += [(3, 0, 3, c, LANES) for c in range(0, coarse_inward[2], LANES)]
    half = coarse_outward[2] // 2
    units += [(4, 0, 1, c, half) for c in (0, half)]
    return units


def gather_scratch(units, split):
    count, lons = len(units), lax.axis_size("lon")
    halves = 2 if split else 1
    dma = pltpu.SemaphoreType.DMA
    return (
        [dma((count,))] + [dma((count, lons - 1, halves))] * 2 + [dma((count, halves))] * 4 + [dma((count,))] * 2
    )


def flat(block):
    return block.reshape(block.shape[0] * block.shape[1], block.shape[2])


def turned(ref, rows, block_of, slots):
    size = ref.shape[1] // slots
    if size % LANES:
        return ref[rows, :]
    return jnp.concatenate(
        [ref[rows, pl.ds(pl.multiple_of(block_of(s) * size, size), size)] for s in range(slots)], axis=1
    )


def turn_back(value, block_of, slots, store):
    size = value.shape[1] // slots
    if size % LANES:
        store(slice(None), value)
        return
    for s in range(slots):
        store(pl.ds(pl.multiple_of(block_of(s) * size, size), size), value[:, s * size : (s + 1) * size])


def tag_rows(plan, tags_ref, column, place, features):
    grid = jnp.concatenate([tags_ref[r].astype(jnp.float32) for r in range(plan.lat_len)], axis=0)
    spots = lax.broadcasted_iota(jnp.int32, (plan.lon_len, features), 0)
    hot = jnp.where(spots == column, 1.0, 0.0).astype(jnp.bfloat16)
    spread = jnp.dot(grid.astype(jnp.bfloat16), hot, preferred_element_type=jnp.float32)
    rows = []
    for q in range(plan.down):
        row = jnp.zeros((1, features), jnp.float32)
        for k in range(HALF_LAT):
            r = q * HALF_LAT + k
            row = jnp.where(place == k, spread[r : r + 1, :], row)
        rows.append(row)
    return jnp.concatenate(rows, axis=0)


def fill_masks(plan, tags, offset, masks):
    lane = lax.broadcasted_iota(jnp.int32, (ROWS, LANES), 1)
    row = lax.broadcasted_iota(jnp.int32, (ROWS, LANES), 0)
    owner = lax.broadcasted_iota(jnp.int32, (1, LANES), 1) // ROWS

    def tag_row(r, c):
        dy = -1 if r < 0 else int(r >= plan.down)
        dx = -1 if c < 0 else int(c >= plan.across)
        side = AROUND.index((dy, dx)) if dy or dx else len(AROUND)
        r, c = r % plan.down, c % plan.across
        return tags[side][r : r + 1, offset + c * LANES : offset + (c + 1) * LANES]

    for q in range(plan.quads):
        r, c = divmod(q, plan.across)
        top, left = r - (r + 1) % 2, c - (c + 1) % 2
        across = tag_row(top, left)
        for a in range(1, 4):
            across = jnp.where(owner == a, tag_row(top + a // 2, left + a % 2), across)
        down = jnp.sum(jnp.where(lane == row, tag_row(r, c), 0.0), axis=-1, keepdims=True)
        masks[q] = jnp.where(down == across, 0.0, -1e30)


def split_table(tables, padded):
    padded[...] = jnp.zeros_like(padded)
    start = 0
    for table in tables:
        heads, entries = table.shape
        padded[start : start + heads, :entries] = table[...] * LOG2E
        start += heads
    rest, terms = padded[...], []
    for _ in range(3):
        term = rest.astype(jnp.bfloat16)
        terms.append(term)
        rest = rest - term.astype(jnp.float32)
    return jnp.concatenate(terms, axis=0)


def fill_bias(parts, number_ref, biases, first, last):
    total = parts.shape[0] // 3
    spots = lax.broadcasted_iota(jnp.int32, (parts.shape[1], LANES), 0)
    for p in range(first, last):
        row = p // QUAD * ROWS + p % QUAD
        hot = jnp.where(spots == number_ref[row : row + 1, :], 1.0, 0.0).astype(jnp.bfloat16)
        terms = jnp.dot(parts, hot, preferred_element_type=jnp.float32)
        value = terms[:total] + terms[total : 2 * total] + terms[2 * total :]
        start = 0
        for bias in biases:
            bias[:, row, :] = value[start : start + bias.shape[0]]
            start += bias.shape[0]


def attend(plan, q, group, query, keys, values, bias_ref, masks, mixed, size):
    heads = LANES // size
    r = lax.div(q, plan.across)
    c = q - r * plan.across
    window = lax.div(r + 1, 2) * plan.columns + lax.div(c + 1, 2)
    place = lax.rem(r + 1, 2) * 2 + lax.rem(c + 1, 2)
    rows = pl.ds(pl.multiple_of(q * ROWS, ROWS), ROWS)
    others = pl.ds(pl.multiple_of(window * WINDOW, WINDOW), WINDOW)
    inside = pl.ds(pl.multiple_of(place * ROWS, ROWS), ROWS)
    cols = slice(group * LANES, (group + 1) * LANES)
    owner = lax.broadcasted_iota(jnp.int32, (ROWS, LANES), 1) // size
    block = query[rows, cols]
    stack = jnp.concatenate([jnp.where(owner == h, block, jnp.zeros_like(block)) for h in range(heads)], axis=0)
    scores = lax.dot_general(stack, keys[others, cols], NT, preferred_element_type=jnp.float32)
    mask = masks[q]
    weights = []
    for h in range(heads):
        score = scores[h * ROWS : (h + 1) * ROWS] + bias_ref[group * heads + h, inside, :] + mask
        weights.append(jnp.exp2(score - jnp.max(score, axis=-1, keepdims=True)).astype(jnp.bfloat16))
    weights = jnp.concatenate(weights, axis=0)
    ones = jnp.ones((WINDOW, LANES), jnp.bfloat16)
    both = jnp.dot(weights, jnp.concatenate([values[others, cols], ones], axis=1), preferred_element_type=jnp.float32)
    result = both[:ROWS]
    blended, totals = result[:, :LANES], result[:, LANES:]
    for h in range(1, heads):
        result = both[h * ROWS : (h + 1) * ROWS]
        blended = jnp.where(owner == h, result[:, :LANES], blended)
        totals = jnp.where(owner == h, result[:, LANES:], totals)
    mixed[rows, cols] = (blended / totals).astype(jnp.bfloat16)


def kernel(
    fine, coarse, units, split, tokens_ref, fine_tags, coarse_tags, fine_gain, merge_gain, coarse_gain, fine_table,
    coarse_table, index_ref, number_ref, lane_ref, s0, s1, s2, s3, s4, fine_ref, coarse_ref,
    tokens, own, wide, query, keys, values, mixed, fine_bias, fine_masks, fine_value,
    two_own, two_wide, two_query, two_keys, two_values, two_mixed, coarse_bias, coarse_masks, two_in, two_value,
    padded, tag_own, tag_wide, f0, f1, f2, f3, f4, local, tag_send, tag_recv, send1, recv1, send2, recv2, *sems,
):
    width, wide_two = tokens.shape[1], two_own.shape[1]
    heads, heads_two = fine_bias.shape[0], coarse_bias.shape[0]
    size = width // heads
    scale = size ** (-0.5) * LOG2E
    around = Around()
    lons, lvls = lax.axis_size("lon"), lax.axis_size("lvl")
    gather = Gather((s0, s1, s2, s3, s4), (f0, f1, f2, f3, f4), units, split, sems)
    block_of = gather.block_of
    fetch = pltpu.make_async_copy(tokens_ref, tokens, local.at[0])
    fetch.start()
    tag_wide[...] = jnp.zeros_like(tag_wide)
    barrier = pltpu.get_barrier_semaphore()
    peers = around.greet(barrier) + gather.greet(barrier)

    fine_lanes = fine.across * LANES
    coarse_lanes = coarse.across * LANES
    tag_own[...] = jnp.zeros_like(tag_own)
    top = tag_rows(fine, fine_tags, lane_ref[0:1, :fine_lanes], lane_ref[1:2, :fine_lanes], fine_lanes)
    tag_own[: fine.down, :fine_lanes] = top.astype(jnp.bfloat16)
    low = tag_rows(coarse, coarse_tags, lane_ref[0:1, fine_lanes:], lane_ref[1:2, fine_lanes:], coarse_lanes)
    tag_own[: coarse.down, fine_lanes:] = low.astype(jnp.bfloat16)
    pl.semaphore_wait(barrier, peers)
    gather.begin()

    def tag_copy(side):
        dy, dx = AROUND[side]
        return around.copy(tag_own, tag_wide.at[side], tag_send.at[side], tag_recv.at[side], dy, dx)

    for side, (dy, dx) in enumerate(AROUND):
        around.when_there(-dy, lambda side=side: tag_copy(side).start())

    fetch.wait()
    normed = normalize(tokens[...], fine_gain[...])
    arranged = pick(index_ref[: fine.quads * ROWS, 0:1], normed)
    own[...] = arranged
    halo = Halo(around, fine, own, wide, send1, recv1)
    halo.start()
    for q in range(fine.quads):
        spot = fine.spot(*divmod(q, fine.across))
        wide[pl.ds(spot * ROWS, ROWS), :] = arranged[q * ROWS : (q + 1) * ROWS]

    parts = split_table((fine_table, coarse_table), padded)
    fine_bias[...] = jnp.zeros_like(fine_bias)
    coarse_bias[...] = jnp.zeros_like(coarse_bias)
    chunk = 4 * QUAD // 4
    for first in range(0, 4 * QUAD, chunk):
        fill_bias(parts, number_ref, (fine_bias, coarse_bias), first, first + chunk)
        gather.step()

    for side, (dy, dx) in enumerate(AROUND):
        around.when_there(dy, lambda side=side: tag_copy(side).wait_recv())
    tags = [tag_wide[side].astype(jnp.float32) for side in range(len(AROUND))] + [tag_own[...].astype(jnp.float32)]
    fill_masks(fine, tags, 0, fine_masks)
    fill_masks(coarse, tags, fine_lanes, coarse_masks)

    gather.ready(0)
    half = width // lvls
    for lvl in range(lvls):
        part = jnp.dot(turned(own, slice(None), block_of, lons), flat(f0[lvl, 0]), preferred_element_type=jnp.float32)
        query[:, lvl * half : (lvl + 1) * half] = (part * scale).astype(jnp.bfloat16)
    halo.finish()
    for member, target in ((1, keys), (2, values)):
        gather.ready(member)

        @pl.loop(0, fine.windows // fine.columns)
        def _(band):
            count = fine.columns * WINDOW
            rows = pl.ds(pl.multiple_of(band * count, count), count)
            x = turned(wide, rows, block_of, lons)
            for lvl in range(lvls):
                part = jnp.dot(x, flat(f0[lvl, member]), preferred_element_type=jnp.float32)
                target[rows, lvl * half : (lvl + 1) * half] = part.astype(jnp.bfloat16)

    per_row = fine.across
    for first in range(0, fine.quads, per_row):
        @pl.loop(first, first + per_row)
        def _(q):
            for group in range(width // LANES):
                attend(fine, q, group, query, keys, values, fine_bias, fine_masks, mixed, size)
        gather.step()

    own_mixed = pick(index_ref[: fine.own, 1:2], mixed[...])
    gather.ready(3)
    update = None
    for lvl in range(lvls):
        term = lax.dot_general(
            own_mixed[:, lvl * half : (lvl + 1) * half], flat(f1[lvl, 0]), NT, preferred_element_type=jnp.float32
        )
        update = term if update is None else update + term

    def put_fine(cols, value):
        fine_value[:, cols] = (tokens[:, cols].astype(jnp.float32) + value).astype(jnp.bfloat16)

    turn_back(update, block_of, lons, put_fine)
    publish = pltpu.make_async_copy(fine_value, fine_ref, local.at[1])
    publish.start()

    count = coarse.quads * ROWS
    stacked = pick(index_ref[: 4 * count, 2:3], fine_value[...]).astype(jnp.float32)
    members = [stacked[m * count : (m + 1) * count] for m in range(4)]
    mean = sum(jnp.sum(m, axis=-1, keepdims=True) for m in members) / (4 * width)
    centers = [m - mean for m in members]
    spread = sum(jnp.sum(c * c, axis=-1, keepdims=True) for c in centers) / (4 * width)
    factor = lax.rsqrt(spread + EPSILON)
    normed = jnp.concatenate(
        [(centers[m] * factor * merge_gain[:, m * width : (m + 1) * width]).astype(jnp.bfloat16) for m in range(4)],
        axis=1,
    )
    merged = None
    share = 4 * width // lvls
    for u in range(4, 8):
        gather.ready(u)
        _, _, _, col, cols = units[u]
        for lvl in range(lvls):
            start = lvl * share + col
            term = lax.dot_general(
                normed[:, start : start + cols], flat(f2[lvl, 0, :, :, col : col + cols]), NT,
                preferred_element_type=jnp.float32,
            )
            merged = term if merged is None else merged + term

    def put_coarse(cols, value):
        two_in[:, cols] = value.astype(jnp.bfloat16)

    turn_back(merged, block_of, lons, put_coarse)
    two_own[...] = normalize(two_in[...], coarse_gain[...])
    halo_two = Halo(around, coarse, two_own, two_wide, send2, recv2)
    halo_two.start()
    for q in range(coarse.quads):
        spot = coarse.spot(*divmod(q, coarse.across))
        two_wide[pl.ds(spot * ROWS, ROWS), :] = two_own[q * ROWS : (q + 1) * ROWS, :]
    gather.step()
    halo_two.finish()

    share = wide_two // lvls
    inner = [u for u in range(len(units)) if units[u][0] == 3]
    for u in inner:
        gather.ready(u)
        _, _, _, col, cols = units[u]
        for lvl in range(lvls):
            start = lvl * share + col
            part = jnp.dot(
                turned(two_own, slice(None), block_of, lons), flat(f3[lvl, 0, :, :, col : col + cols]),
                preferred_element_type=jnp.float32,
            )
            two_query[:, start : start + cols] = (part * scale).astype(jnp.bfloat16)
            weight = jnp.concatenate([flat(f3[lvl, k, :, :, col : col + cols]) for k in (1, 2)], axis=1)
            part = jnp.dot(
                turned(two_wide, slice(None), block_of, lons), weight, preferred_element_type=jnp.float32
            ).astype(jnp.bfloat16)
            two_keys[:, start : start + cols] = part[:, :cols]
            two_values[:, start : start + cols] = part[:, cols:]

        @pl.loop(0, coarse.quads)
        def _(q):
            for lvl in range(lvls):
                group = (lvl * share + col) // LANES
                attend(coarse, q, group, two_query, two_keys, two_values, coarse_bias, coarse_masks, two_mixed, size)

    update = None
    for u in [u for u in range(len(units)) if units[u][0] == 4]:
        gather.ready(u)
        _, _, _, col, cols = units[u]
        for lvl in range(lvls):
            start = lvl * share + col
            term = lax.dot_general(
                two_mixed[:, start : start + cols], flat(f4[lvl, 0, :, :, col : col + cols]), NT,
                preferred_element_type=jnp.float32,
            )
            update = term if update is None else update + term

    def put_out(cols, value):
        two_value[:, cols] = (two_in[:, cols].astype(jnp.float32) + value).astype(jnp.bfloat16)

    turn_back(update, block_of, lons, put_out)
    pitch = up_to(coarse.lon_len, 16)
    result = pick(index_ref[: coarse.lat_len * pitch, 3:4], two_value[...])
    for r in range(coarse.lat_len):
        coarse_ref[r] = result[r * pitch : r * pitch + coarse.lon_len]

    publish.wait()
    gather.end()
    for side, (dy, dx) in enumerate(AROUND):
        around.when_there(-dy, lambda side=side: tag_copy(side).wait_send())
    halo.drain()
    halo_two.drain()


def level_scratch(plan, features, heads):
    rows, all_rows = plan.quads * ROWS, plan.windows * WINDOW
    return [
        pltpu.VMEM((rows, features), jnp.bfloat16),
        pltpu.VMEM((all_rows, features), jnp.bfloat16),
        pltpu.VMEM((rows, features), jnp.bfloat16),
        pltpu.VMEM((all_rows, features), jnp.bfloat16),
        pltpu.VMEM((all_rows, features), jnp.bfloat16),
        pltpu.VMEM((rows, features), jnp.bfloat16),
        pltpu.VMEM((heads, WINDOW, LANES), jnp.float32),
        pltpu.VMEM((plan.quads, ROWS, LANES), jnp.float32),
    ]


def shards(
    tokens, fine_tags, coarse_tags, fine_gain, fine_inward, fine_outward, fine_table, merge_gain,
    merge_weight, coarse_gain, coarse_inward, coarse_outward, coarse_table,
):
    _, lat_len, lon_len, width = tokens.shape
    fine, coarse = Plan(lat_len, lon_len), Plan(lat_len // 2, lon_len // 2)
    weights = [fine_inward, fine_outward[None], merge_weight[None], coarse_inward, coarse_outward[None]]
    grps, lats, lons, lvls = (lax.axis_size(a) for a in ("grp", "lat", "lon", "lvl"))
    split = grps == 2 and lats == 2 and all(w.shape[1] % LANES == 0 for w in weights)
    units = weight_units(weights)
    wide_two = coarse_inward.shape[1] * lons
    heads, heads_two = fine_table.shape[0], coarse_table.shape[0]
    pitch = up_to(coarse.lon_len, 16)

    columns = [fine.natural(), fine.back(fine.lon_len), patches(fine, coarse), coarse.back(pitch)]
    index = np.full((max(len(c) for c in columns), len(columns)), -1, np.int32)
    for n, column in enumerate(columns):
        index[: len(column), n] = column
    lane = np.concatenate([np.stack(p.lanes()) for p in (fine, coarse)], axis=1).astype(np.int32)

    dma = pltpu.SemaphoreType.DMA
    bf16 = jnp.bfloat16
    sides = len(AROUND)
    fine_out, coarse_out = pl.pallas_call(
        functools.partial(kernel, fine, coarse, units, split),
        out_shape=[
            jax.ShapeDtypeStruct((fine.own, width), bf16),
            jax.ShapeDtypeStruct((coarse.lat_len, coarse.lon_len, wide_two), bf16),
        ],
        in_specs=[ANY] + [VMEM] * 10 + [ANY] * 5,
        out_specs=[ANY, VMEM],
        scratch_shapes=[pltpu.VMEM((fine.own, width), bf16)]
        + level_scratch(fine, width, heads)
        + [pltpu.VMEM((fine.own, width), bf16)]
        + level_scratch(coarse, wide_two, heads_two)
        + [pltpu.VMEM((coarse.quads * ROWS, wide_two), bf16)] * 2
        + [
            pltpu.VMEM((heads + heads_two, up_to(fine_table.shape[1], LANES)), jnp.float32),
            pltpu.VMEM((16, lane.shape[1]), bf16),
            pltpu.VMEM((sides, 16, lane.shape[1]), bf16),
        ]
        + [pltpu.VMEM((lvls, w.shape[0], lons, w.shape[1], w.shape[2]), bf16) for w in weights]
        + [dma((2,)), dma((sides,)), dma((sides,))]
        + [dma((len(fine.halo),))] * 2
        + [dma((len(coarse.halo),))] * 2
        + gather_scratch(units, split),
        compiler_params=pltpu.CompilerParams(collective_id=1, has_side_effects=True, vmem_limit_bytes=LIMIT),
        name="levels",
    )(
        tokens.reshape(fine.own, width), fine_tags.reshape(lat_len, 1, lon_len),
        coarse_tags.reshape(coarse.lat_len, 1, coarse.lon_len), fine_gain[None], merge_gain[None], coarse_gain[None],
        fine_table, coarse_table, index, offset_numbers(), lane, *weights,
    )
    return fine_out.reshape(tokens.shape), coarse_out[None]


def solution(mesh):
    placed = (
        P(("grp", "lvl"), "lat", "lon", None),
        P(("grp", "lvl"), "lat", "lon"),
        P(("grp", "lvl"), "lat", "lon"),
        P(),
        P(None, "lon", "lvl"),
        P("lon", "lvl"),
        P(),
        P(),
        P("lon", "lvl"),
        P(),
        P(None, "lon", "lvl"),
        P("lon", "lvl"),
        P(),
    )
    return jax.shard_map(
        shards,
        mesh=mesh,
        in_specs=placed,
        out_specs=(P(("grp", "lvl"), "lat", "lon", None), P(("grp", "lvl"), "lat", "lon", None)),
        check_vma=False,
    )
```

```python
import functools
import math

import jax
import jax.numpy as jnp
import numpy as np
from jax import lax
from jax.experimental import pallas as pl
from jax.experimental.pallas import tpu as pltpu
from jax.sharding import PartitionSpec as P

WIN_LAT = 6
WIN_LON = 12
HALF_LAT = WIN_LAT // 2
HALF_LON = WIN_LON // 2
QUAD = HALF_LAT * HALF_LON
ROWS = -(-QUAD // 16) * 16
SENT = -(-QUAD // 8) * 8
WINDOW = 4 * ROWS
EPSILON = 1e-05
LANES = 128
LOG2E = math.log2(math.e)
MESH = pl.DeviceIdType.MESH
VMEM = pl.BlockSpec(memory_space=pltpu.VMEM)
ANY = pl.BlockSpec(memory_space=pl.ANY)
LIMIT = 60 * 1024 * 1024
NT = (((1,), (1,)), ((), ()))
AROUND = ((0, -1), (0, 1), (-1, 0), (1, 0), (-1, -1), (-1, 1), (1, -1), (1, 1))
AHEAD = 2


def up_to(count, step):
    return -(-count // step) * step


class Plan:
    def __init__(self, lat_len, lon_len):
        self.lat_len, self.lon_len = lat_len, lon_len
        self.own = lat_len * lon_len
        self.down, self.across = lat_len // HALF_LAT, lon_len // HALF_LON
        self.quads = self.down * self.across
        self.columns = self.across // 2 + 1
        self.windows = (self.down // 2 + 1) * self.columns
        self.halo = []
        for side, (dy, dx) in enumerate(AROUND):
            rows = [-1] if dy < 0 else ([self.down] if dy > 0 else range(self.down))
            cols = [-1] if dx < 0 else ([self.across] if dx > 0 else range(self.across))
            for r in rows:
                for c in cols:
                    self.halo.append((side, r, c, (r % self.down) * self.across + c % self.across))

    def spot(self, r, c):
        window = ((r + 1) // 2) * self.columns + (c + 1) // 2
        return 4 * window + ((r + 1) % 2) * 2 + (c + 1) % 2

    def natural(self):
        result = np.full((self.quads * ROWS,), -1, np.int32)
        for q in range(self.quads):
            for p in range(QUAD):
                r = (q // self.across) * HALF_LAT + p // HALF_LON
                c = (q % self.across) * HALF_LON + p % HALF_LON
                result[q * ROWS + p] = r * self.lon_len + c
        return result

    def back(self, pitch):
        result = np.full((self.lat_len * pitch,), -1, np.int32)
        for row, token in enumerate(self.natural()):
            if token >= 0:
                result[token // self.lon_len * pitch + token % self.lon_len] = row
        return result

    def lanes(self):
        lane = np.arange(self.across * LANES)
        place = lane % ROWS
        column = (lane // LANES) * HALF_LON + place % HALF_LON
        return np.where(place < QUAD, column, -1), np.where(place < QUAD, place // HALF_LON, -1)


def patches(fine, coarse):
    token = coarse.natural()
    result = []
    for s in range(2):
        for t in range(2):
            a, b = token // coarse.lon_len, token % coarse.lon_len
            result.append(np.where(token >= 0, (2 * a + s) * fine.lon_len + 2 * b + t, -1))
    return np.concatenate(result)


def offset_numbers():
    spot = np.arange(WINDOW)
    place = spot % ROWS
    r = spot // ROWS // 2 * HALF_LAT + place // HALF_LON
    c = spot // ROWS % 2 * HALF_LON + place % HALF_LON
    number = (r[:, None] - r[None, :] + WIN_LAT - 1) * (2 * WIN_LON - 1) + c[:, None] - c[None, :] + WIN_LON - 1
    valid = (place < QUAD)[:, None] & (place < QUAD)[None, :]
    return np.where(valid, number, -1).astype(np.int32)


def onehot(index, width):
    spots = lax.broadcasted_iota(jnp.int32, (index.shape[0], width), 1)
    return jnp.where(spots == index, 1.0, 0.0).astype(jnp.bfloat16)


def pick(index, source):
    return jnp.dot(
        onehot(index, source.shape[0]), source, preferred_element_type=jnp.float32
    ).astype(jnp.bfloat16)


def normalize(values, gain):
    widened = values.astype(jnp.float32)
    center = widened - jnp.mean(widened, axis=-1, keepdims=True)
    spread = jnp.mean(center * center, axis=-1, keepdims=True)
    return (center * lax.rsqrt(spread + EPSILON) * gain).astype(jnp.bfloat16)


class Around:
    def __init__(self):
        self.lat, self.lon = lax.axis_index("lat"), lax.axis_index("lon")
        self.lats, self.lons = lax.axis_size("lat"), lax.axis_size("lon")

    def place(self, dy, dx):
        return {
            "lat": lax.rem(self.lat + dy + self.lats, self.lats),
            "lon": lax.rem(self.lon + dx + self.lons, self.lons),
        }

    def there(self, dy):
        return (self.lat > 0) if dy < 0 else (self.lat < self.lats - 1)

    def when_there(self, dy, action):
        if dy == 0:
            action()
        else:
            pl.when(self.there(dy))(action)

    def greet(self, barrier):
        for dy, dx in AROUND:
            def signal(dy=dy, dx=dx):
                pl.semaphore_signal(barrier, inc=1, device_id=self.place(dy, dx), device_id_type=MESH)
            self.when_there(dy, signal)
        return 2 + 3 * (self.lat > 0).astype(jnp.int32) + 3 * (self.lat < self.lats - 1).astype(jnp.int32)

    def copy(self, src, dst, send, recv, dy, dx):
        return pltpu.make_async_remote_copy(
            src_ref=src, dst_ref=dst, send_sem=send, recv_sem=recv,
            device_id=self.place(-dy, -dx), device_id_type=MESH,
        )


class Halo:
    def __init__(self, around, plan, own, wide, send, recv):
        self.around, self.plan, self.own, self.wide, self.send, self.recv = around, plan, own, wide, send, recv

    def copy(self, n):
        side, r, c, q = self.plan.halo[n]
        return self.around.copy(
            self.own.at[pl.ds(q * ROWS, SENT)], self.wide.at[pl.ds(self.plan.spot(r, c) * ROWS, SENT)],
            self.send.at[n], self.recv.at[n], *AROUND[side],
        )

    def clear(self):
        for _, r, c, _ in self.plan.halo:
            rows = pl.ds(self.plan.spot(r, c) * ROWS, ROWS)
            self.wide[rows, :] = jnp.zeros((ROWS, self.wide.shape[1]), self.wide.dtype)

    def start(self):
        for n, (side, *_) in enumerate(self.plan.halo):
            self.around.when_there(-AROUND[side][0], lambda n=n: self.copy(n).start())

    def finish(self):
        for n, (side, *_) in enumerate(self.plan.halo):
            self.around.when_there(AROUND[side][0], lambda n=n: self.copy(n).wait_recv())

    def drain(self):
        for n, (side, *_) in enumerate(self.plan.halo):
            self.around.when_there(-AROUND[side][0], lambda n=n: self.copy(n).wait_send())


class Gather:
    def __init__(self, shards, fulls, units, split, sems):
        self.shards, self.fulls, self.units, self.split, self.sems = shards, fulls, units, split, sems
        self.index = {a: lax.axis_index(a) for a in ("grp", "lat", "lon", "lvl")}
        self.size = {a: lax.axis_size(a) for a in ("grp", "lat", "lon", "lvl")}
        self.halves = range(2 if split else 1)
        self.ways = [(s, half) for s in range(1, self.size["lon"]) for half in self.halves]
        self.now = 0
        self.steps = len(units) + (2 if split else 0)

    def at(self, axis, step):
        return {axis: lax.rem(self.index[axis] + step + self.size[axis], self.size[axis])}

    def greet(self, barrier):
        peers = 0
        for axis in ("lon", "lvl", "lat", "grp") if self.split else ("lon", "lvl"):
            for d in range(1, self.size[axis]):
                pl.semaphore_signal(barrier, inc=1, device_id=self.at(axis, d), device_id_type=MESH)
                peers += 1
        return peers

    def block_of(self, slot):
        return lax.rem(self.index["lon"] + slot, self.size["lon"]) if self.split else slot

    def rows(self, u):
        return self.shards[self.units[u][0]].shape[1]

    def axes(self, half):
        return ("lat", "grp") if half == 0 else ("grp", "lat")

    def piece(self, u, half):
        if not self.split:
            return 0, self.rows(u)
        size = self.rows(u) // 8
        first, second = self.axes(half)
        order = self.index[second] * 2 + self.index[first]
        return pl.multiple_of((half * 4 + order) * size, 16), size

    def pair(self, u, half):
        size = self.rows(u) // 8
        return pl.multiple_of((half * 4 + self.index[self.axes(half)[1]] * 2) * size, 16), 2 * size

    def held(self, u, start, size):
        m, k, depth, col, cols = self.units[u]
        return self.shards[m].at[pl.ds(k, depth), pl.ds(start, size), pl.ds(col, cols)]

    def block(self, u, slot, slots, start, size):
        m, k, depth, col, cols = self.units[u]
        return self.fulls[m].at[
            self.index["lvl"], pl.ds(k, depth), pl.ds(slot, slots), pl.ds(start, size), pl.ds(col, cols)
        ]

    def slot(self, u, slot, start, size):
        m, k, depth, col, cols = self.units[u]
        return self.fulls[m].at[self.index["lvl"], pl.ds(k, depth), slot, pl.ds(start, size), pl.ds(col, cols)]

    def remote(self, src, dst, kind, number, device):
        send, recv = self.sems[1 + 2 * kind], self.sems[2 + 2 * kind]
        return pltpu.make_async_remote_copy(
            src_ref=src, dst_ref=dst, send_sem=send.at[number], recv_sem=recv.at[number],
            device_id=device, device_id_type=MESH,
        )

    def own_copy(self, u):
        slot = 0 if self.split else self.index["lon"]
        return pltpu.make_async_copy(
            self.held(u, 0, self.rows(u)), self.slot(u, slot, 0, self.rows(u)), self.sems[0].at[u]
        )

    def lon_copy(self, u, s, half):
        start, size = self.piece(u, half)
        slot = s if self.split else self.index["lon"]
        return self.remote(
            self.held(u, start, size), self.slot(u, slot, start, size), 0, (u, s - 1, half), self.at("lon", -s)
        )

    def one_copy(self, u, half):
        block = self.block(u, 1, self.size["lon"] - 1, *self.piece(u, half))
        return self.remote(block, block, 1, (u, half), self.at(self.axes(half)[0], 1))

    def two_copy(self, u, half):
        block = self.block(u, 1, self.size["lon"] - 1, *self.pair(u, half))
        return self.remote(block, block, 2, (u, half), self.at(self.axes(half)[1], 1))

    def lvl_copy(self, u):
        block = self.block(u, 0, self.size["lon"], 0, self.rows(u))
        return self.remote(block, block, 3, (u,), self.at("lvl", 1))

    def issue(self, u):
        if u < len(self.units):
            for s, half in self.ways:
                self.lon_copy(u, s, half).start()
            self.own_copy(u).start()

    def begin(self):
        for u in range(AHEAD):
            self.issue(u)

    def step(self):
        k, count = self.now, len(self.units)
        self.now += 1
        if k < count:
            for half in self.halves:
                for s in range(1, self.size["lon"]):
                    self.lon_copy(k, s, half).wait_recv()
                if self.split:
                    self.one_copy(k, half).start()
            self.issue(k + AHEAD)
        if self.split and 0 <= k - 1 < count:
            for half in self.halves:
                self.one_copy(k - 1, half).wait_recv()
                self.two_copy(k - 1, half).start()
        done = k - 2 if self.split else k
        if 0 <= done < count:
            if self.split:
                for half in self.halves:
                    self.two_copy(done, half).wait_recv()
            self.own_copy(done).wait()
            self.lvl_copy(done).start()

    def ready(self, *wanted):
        for u in wanted:
            while self.now <= u + (2 if self.split else 0):
                self.step()
            self.lvl_copy(u).wait_recv()

    def end(self):
        for u in range(len(self.units)):
            self.lvl_copy(u).wait_send()
            for s, half in self.ways:
                self.lon_copy(u, s, half).wait_send()
            if self.split:
                for half in self.halves:
                    self.one_copy(u, half).wait_send()
                    self.two_copy(u, half).wait_send()


def weight_units(shards):
    fine_inward, fine_outward, merge, coarse_inward, coarse_outward = [s.shape for s in shards]
    units = [(0, k, 1, 0, fine_inward[2]) for k in range(3)]
    units.append((1, 0, 1, 0, fine_outward[2]))
    units += [(2, 0, 1, c, merge[2] // 4) for c in range(0, merge[2], merge[2] // 4)]
    units += [(3, 0, 3, c, LANES) for c in range(0, coarse_inward[2], LANES)]
    half = coarse_outward[2] // 2
    units += [(4, 0, 1, c, half) for c in (0, half)]
    return units


def gather_scratch(units, split):
    count, lons = len(units), lax.axis_size("lon")
    halves = 2 if split else 1
    dma = pltpu.SemaphoreType.DMA
    return (
        [dma((count,))] + [dma((count, lons - 1, halves))] * 2 + [dma((count, halves))] * 4 + [dma((count,))] * 2
    )


def flat(block):
    return block.reshape(block.shape[0] * block.shape[1], block.shape[2])


def turned(ref, rows, block_of, slots):
    size = ref.shape[1] // slots
    if size % LANES:
        return ref[rows, :]
    return jnp.concatenate(
        [ref[rows, pl.ds(pl.multiple_of(block_of(s) * size, size), size)] for s in range(slots)], axis=1
    )


def turn_back(value, block_of, slots, store):
    size = value.shape[1] // slots
    if size % LANES:
        store(slice(None), value)
        return
    for s in range(slots):
        store(pl.ds(pl.multiple_of(block_of(s) * size, size), size), value[:, s * size : (s + 1) * size])


def tag_rows(plan, tags_ref, column, place, features):
    grid = jnp.concatenate([tags_ref[r].astype(jnp.float32) for r in range(plan.lat_len)], axis=0)
    spots = lax.broadcasted_iota(jnp.int32, (plan.lon_len, features), 0)
    hot = jnp.where(spots == column, 1.0, 0.0).astype(jnp.bfloat16)
    spread = jnp.dot(grid.astype(jnp.bfloat16), hot, preferred_element_type=jnp.float32)
    rows = []
    for q in range(plan.down):
        row = jnp.zeros((1, features), jnp.float32)
        for k in range(HALF_LAT):
            r = q * HALF_LAT + k
            row = jnp.where(place == k, spread[r : r + 1, :], row)
        rows.append(row)
    return jnp.concatenate(
        [row[:, c * LANES : (c + 1) * LANES] for row in rows for c in range(plan.across)], axis=0
    )


def fill_masks(plan, tags, offset, masks):
    lane = lax.broadcasted_iota(jnp.int32, (ROWS, LANES), 1)
    row = lax.broadcasted_iota(jnp.int32, (ROWS, LANES), 0)
    owner = lax.broadcasted_iota(jnp.int32, (1, LANES), 1) // ROWS

    def tag_row(r, c):
        dy = -1 if r < 0 else int(r >= plan.down)
        dx = -1 if c < 0 else int(c >= plan.across)
        side = AROUND.index((dy, dx)) if dy or dx else len(AROUND)
        row = offset + r % plan.down * plan.across + c % plan.across
        return tags[side][row : row + 1]

    for q in range(plan.quads):
        r, c = divmod(q, plan.across)
        top, left = r - (r + 1) % 2, c - (c + 1) % 2
        across = tag_row(top, left)
        for a in range(1, 4):
            across = jnp.where(owner == a, tag_row(top + a // 2, left + a % 2), across)
        down = jnp.sum(jnp.where(lane == row, tag_row(r, c), 0.0), axis=-1, keepdims=True)
        masks[q] = jnp.where(down == across, 0.0, -1e30)


def split_table(tables, padded):
    padded[...] = jnp.zeros_like(padded)
    start = 0
    for table in tables:
        heads, entries = table.shape
        padded[start : start + heads, :entries] = table[...] * LOG2E
        start += heads
    rest, terms = padded[...], []
    for _ in range(3):
        term = rest.astype(jnp.bfloat16)
        terms.append(term)
        rest = rest - term.astype(jnp.float32)
    return jnp.concatenate(terms, axis=0)


def fill_bias(parts, number_ref, biases, first, last):
    total = parts.shape[0] // 3
    spots = lax.broadcasted_iota(jnp.int32, (parts.shape[1], LANES), 0)
    for p in range(first, last):
        row = p // QUAD * ROWS + p % QUAD
        hot = jnp.where(spots == number_ref[row : row + 1, :], 1.0, 0.0).astype(jnp.bfloat16)
        terms = jnp.dot(parts, hot, preferred_element_type=jnp.float32)
        value = terms[:total] + terms[total : 2 * total] + terms[2 * total :]
        start = 0
        for bias in biases:
            bias[:, row, :] = value[start : start + bias.shape[0]]
            start += bias.shape[0]


def attend(plan, spots, query, keys, values, bias_ref, masks, mixed, size):
    heads = LANES // size
    owner = lax.broadcasted_iota(jnp.int32, (ROWS, LANES), 1) // size
    ones = jnp.ones((WINDOW, LANES), jnp.bfloat16)
    where, scores, weights, both = [], [], [], []
    for q, group in spots:
        r = lax.div(q, plan.across)
        c = q - r * plan.across
        window = lax.div(r + 1, 2) * plan.columns + lax.div(c + 1, 2)
        place = lax.rem(r + 1, 2) * 2 + lax.rem(c + 1, 2)
        where.append((
            q, group, pl.ds(pl.multiple_of(q * ROWS, ROWS), ROWS), pl.ds(pl.multiple_of(window * WINDOW, WINDOW), WINDOW),
            pl.ds(pl.multiple_of(place * ROWS, ROWS), ROWS), slice(group * LANES, (group + 1) * LANES),
        ))
    for q, group, rows, others, inside, cols in where:
        block = query[rows, cols]
        stack = jnp.concatenate([jnp.where(owner == h, block, jnp.zeros_like(block)) for h in range(heads)], axis=0)
        scores.append(lax.dot_general(stack, keys[others, cols], NT, preferred_element_type=jnp.float32))
    for (q, group, rows, others, inside, cols), score in zip(where, scores):
        bias = bias_ref[group * heads : (group + 1) * heads, inside, :].reshape(heads * ROWS, LANES)
        score = score + bias + jnp.concatenate([masks[q]] * heads, axis=0)
        weights.append(jnp.exp2(score - jnp.max(score, axis=-1, keepdims=True)).astype(jnp.bfloat16))
    for (q, group, rows, others, inside, cols), weight in zip(where, weights):
        both.append(jnp.dot(
            weight, jnp.concatenate([values[others, cols], ones], axis=1), preferred_element_type=jnp.float32
        ))
    for (q, group, rows, others, inside, cols), part in zip(where, both):
        blended, totals = part[:ROWS, :LANES], part[:ROWS, LANES:]
        for h in range(1, heads):
            result = part[h * ROWS : (h + 1) * ROWS]
            blended = jnp.where(owner == h, result[:, :LANES], blended)
            totals = jnp.where(owner == h, result[:, LANES:], totals)
        mixed[rows, cols] = (blended / totals).astype(jnp.bfloat16)


def kernel(
    fine, coarse, units, split, tokens_ref, fine_tags, coarse_tags, fine_gain, merge_gain, coarse_gain, fine_table,
    coarse_table, index_ref, number_ref, lane_ref, s0, s1, s2, s3, s4, fine_ref, coarse_ref,
    tokens, own, wide, query, keys, values, mixed, fine_bias, fine_masks, fine_value,
    two_own, two_wide, two_query, two_keys, two_values, two_mixed, coarse_bias, coarse_masks, two_in, two_value,
    padded, tag_own, tag_wide, f0, f1, f2, f3, f4, local, tag_send, tag_recv, send1, recv1, send2, recv2, *sems,
):
    width, wide_two = tokens.shape[1], two_own.shape[1]
    heads, heads_two = fine_bias.shape[0], coarse_bias.shape[0]
    size = width // heads
    scale = size ** (-0.5) * LOG2E
    around = Around()
    lons, lvls = lax.axis_size("lon"), lax.axis_size("lvl")
    gather = Gather((s0, s1, s2, s3, s4), (f0, f1, f2, f3, f4), units, split, sems)
    block_of = gather.block_of
    fetch = pltpu.make_async_copy(tokens_ref, tokens, local.at[0])
    fetch.start()
    tag_wide[...] = jnp.zeros_like(tag_wide)
    halo = Halo(around, fine, own, wide, send1, recv1)
    halo_two = Halo(around, coarse, two_own, two_wide, send2, recv2)
    halo.clear()
    halo_two.clear()
    barrier = pltpu.get_barrier_semaphore()
    peers = around.greet(barrier) + gather.greet(barrier)

    fine_lanes = fine.across * LANES
    coarse_lanes = coarse.across * LANES
    top = tag_rows(fine, fine_tags, lane_ref[0:1, :fine_lanes], lane_ref[1:2, :fine_lanes], fine_lanes)
    spare = jnp.zeros((tag_own.shape[0] - fine.quads - coarse.quads, LANES), jnp.float32)
    low = tag_rows(coarse, coarse_tags, lane_ref[0:1, fine_lanes:], lane_ref[1:2, fine_lanes:], coarse_lanes)
    tag_own[...] = jnp.concatenate([top, low, spare], axis=0).astype(jnp.bfloat16)
    pl.semaphore_wait(barrier, peers)
    gather.begin()

    def tag_copy(side):
        dy, dx = AROUND[side]
        return around.copy(tag_own, tag_wide.at[side], tag_send.at[side], tag_recv.at[side], dy, dx)

    for side, (dy, dx) in enumerate(AROUND):
        around.when_there(-dy, lambda side=side: tag_copy(side).start())

    fetch.wait()
    normed = normalize(tokens[...], fine_gain[...])
    arranged = pick(index_ref[: fine.quads * ROWS, 0:1], normed)
    own[...] = arranged
    halo.start()
    for q in range(fine.quads):
        spot = fine.spot(*divmod(q, fine.across))
        wide[pl.ds(spot * ROWS, ROWS), :] = arranged[q * ROWS : (q + 1) * ROWS]

    parts = split_table((fine_table, coarse_table), padded)
    fine_bias[...] = jnp.zeros_like(fine_bias)
    coarse_bias[...] = jnp.zeros_like(coarse_bias)
    chunk = 4 * QUAD // 4
    for first in range(0, 4 * QUAD, chunk):
        fill_bias(parts, number_ref, (fine_bias, coarse_bias), first, first + chunk)
        gather.step()

    for side, (dy, dx) in enumerate(AROUND):
        around.when_there(dy, lambda side=side: tag_copy(side).wait_recv())
    tags = [tag_wide[side].astype(jnp.float32) for side in range(len(AROUND))] + [tag_own[...].astype(jnp.float32)]
    fill_masks(fine, tags, 0, fine_masks)
    fill_masks(coarse, tags, fine.quads, coarse_masks)

    gather.ready(0)
    half = width // lvls
    for lvl in range(lvls):
        part = jnp.dot(turned(own, slice(None), block_of, lons), flat(f0[lvl, 0]), preferred_element_type=jnp.float32)
        query[:, lvl * half : (lvl + 1) * half] = (part * scale).astype(jnp.bfloat16)
    halo.finish()
    for member, target in ((1, keys), (2, values)):
        gather.ready(member)

        @pl.loop(0, fine.windows // fine.columns)
        def _(band):
            count = fine.columns * WINDOW
            rows = pl.ds(pl.multiple_of(band * count, count), count)
            x = turned(wide, rows, block_of, lons)
            for lvl in range(lvls):
                part = jnp.dot(x, flat(f0[lvl, member]), preferred_element_type=jnp.float32)
                target[rows, lvl * half : (lvl + 1) * half] = part.astype(jnp.bfloat16)

    per_row = fine.across
    for first in range(0, fine.quads, per_row):
        @pl.loop(first, first + per_row, step=2)
        def _(q):
            attend(
                fine, [(q + i, group) for i in range(2) for group in range(width // LANES)], query, keys, values,
                fine_bias, fine_masks, mixed, size,
            )
        gather.step()

    own_mixed = pick(index_ref[: fine.own, 1:2], mixed[...])
    gather.ready(3)
    update = None
    for lvl in range(lvls):
        term = lax.dot_general(
            own_mixed[:, lvl * half : (lvl + 1) * half], flat(f1[lvl, 0]), NT, preferred_element_type=jnp.float32
        )
        update = term if update is None else update + term

    def put_fine(cols, value):
        fine_value[:, cols] = (tokens[:, cols].astype(jnp.float32) + value).astype(jnp.bfloat16)

    turn_back(update, block_of, lons, put_fine)
    publish = pltpu.make_async_copy(fine_value, fine_ref, local.at[1])
    publish.start()

    count = coarse.quads * ROWS
    stacked = pick(index_ref[: 4 * count, 2:3], fine_value[...]).astype(jnp.float32)
    members = [stacked[m * count : (m + 1) * count] for m in range(4)]
    mean = sum(jnp.sum(m, axis=-1, keepdims=True) for m in members) / (4 * width)
    centers = [m - mean for m in members]
    spread = sum(jnp.sum(c * c, axis=-1, keepdims=True) for c in centers) / (4 * width)
    factor = lax.rsqrt(spread + EPSILON)
    normed = jnp.concatenate(
        [(centers[m] * factor * merge_gain[:, m * width : (m + 1) * width]).astype(jnp.bfloat16) for m in range(4)],
        axis=1,
    )
    merged = None
    share = 4 * width // lvls
    for u in range(4, 8):
        gather.ready(u)
        _, _, _, col, cols = units[u]
        for lvl in range(lvls):
            start = lvl * share + col
            term = lax.dot_general(
                normed[:, start : start + cols], flat(f2[lvl, 0, :, :, col : col + cols]), NT,
                preferred_element_type=jnp.float32,
            )
            merged = term if merged is None else merged + term

    def put_coarse(cols, value):
        two_in[:, cols] = value.astype(jnp.bfloat16)

    turn_back(merged, block_of, lons, put_coarse)
    two_own[...] = normalize(two_in[...], coarse_gain[...])
    halo_two.start()
    for q in range(coarse.quads):
        spot = coarse.spot(*divmod(q, coarse.across))
        two_wide[pl.ds(spot * ROWS, ROWS), :] = two_own[q * ROWS : (q + 1) * ROWS, :]
    gather.step()
    halo_two.finish()

    share = wide_two // lvls
    inner = [u for u in range(len(units)) if units[u][0] == 3]
    for u in inner:
        gather.ready(u)
        _, _, _, col, cols = units[u]
        for lvl in range(lvls):
            start = lvl * share + col
            part = jnp.dot(
                turned(two_own, slice(None), block_of, lons), flat(f3[lvl, 0, :, :, col : col + cols]),
                preferred_element_type=jnp.float32,
            )
            two_query[:, start : start + cols] = (part * scale).astype(jnp.bfloat16)
            weight = jnp.concatenate([flat(f3[lvl, k, :, :, col : col + cols]) for k in (1, 2)], axis=1)
            part = jnp.dot(
                turned(two_wide, slice(None), block_of, lons), weight, preferred_element_type=jnp.float32
            ).astype(jnp.bfloat16)
            two_keys[:, start : start + cols] = part[:, :cols]
            two_values[:, start : start + cols] = part[:, cols:]

        attend(
            coarse, [(q, (lvl * share + col) // LANES) for q in range(coarse.quads) for lvl in range(lvls)],
            two_query, two_keys, two_values, coarse_bias, coarse_masks, two_mixed, size,
        )

    update = None
    for u in [u for u in range(len(units)) if units[u][0] == 4]:
        gather.ready(u)
        _, _, _, col, cols = units[u]
        for lvl in range(lvls):
            start = lvl * share + col
            term = lax.dot_general(
                two_mixed[:, start : start + cols], flat(f4[lvl, 0, :, :, col : col + cols]), NT,
                preferred_element_type=jnp.float32,
            )
            update = term if update is None else update + term

    def put_out(cols, value):
        two_value[:, cols] = (two_in[:, cols].astype(jnp.float32) + value).astype(jnp.bfloat16)

    turn_back(update, block_of, lons, put_out)
    pitch = up_to(coarse.lon_len, 16)
    result = pick(index_ref[: coarse.lat_len * pitch, 3:4], two_value[...])
    for r in range(coarse.lat_len):
        coarse_ref[r] = result[r * pitch : r * pitch + coarse.lon_len]

    publish.wait()
    gather.end()
    for side, (dy, dx) in enumerate(AROUND):
        around.when_there(-dy, lambda side=side: tag_copy(side).wait_send())
    halo.drain()
    halo_two.drain()


def level_scratch(plan, features, heads):
    rows, all_rows = plan.quads * ROWS, plan.windows * WINDOW
    return [
        pltpu.VMEM((rows, features), jnp.bfloat16),
        pltpu.VMEM((all_rows, features), jnp.bfloat16),
        pltpu.VMEM((rows, features), jnp.bfloat16),
        pltpu.VMEM((all_rows, features), jnp.bfloat16),
        pltpu.VMEM((all_rows, features), jnp.bfloat16),
        pltpu.VMEM((rows, features), jnp.bfloat16),
        pltpu.VMEM((heads, WINDOW, LANES), jnp.float32),
        pltpu.VMEM((plan.quads, ROWS, LANES), jnp.float32),
    ]


def shards(
    tokens, fine_tags, coarse_tags, fine_gain, fine_inward, fine_outward, fine_table, merge_gain,
    merge_weight, coarse_gain, coarse_inward, coarse_outward, coarse_table,
):
    _, lat_len, lon_len, width = tokens.shape
    fine, coarse = Plan(lat_len, lon_len), Plan(lat_len // 2, lon_len // 2)
    weights = [fine_inward, fine_outward[None], merge_weight[None], coarse_inward, coarse_outward[None]]
    grps, lats, lons, lvls = (lax.axis_size(a) for a in ("grp", "lat", "lon", "lvl"))
    split = grps == 2 and lats == 2 and all(w.shape[1] % LANES == 0 for w in weights)
    units = weight_units(weights)
    wide_two = coarse_inward.shape[1] * lons
    heads, heads_two = fine_table.shape[0], coarse_table.shape[0]
    pitch = up_to(coarse.lon_len, 16)

    columns = [fine.natural(), fine.back(fine.lon_len), patches(fine, coarse), coarse.back(pitch)]
    index = np.full((max(len(c) for c in columns), len(columns)), -1, np.int32)
    for n, column in enumerate(columns):
        index[: len(column), n] = column
    lane = np.concatenate([np.stack(p.lanes()) for p in (fine, coarse)], axis=1).astype(np.int32)

    dma = pltpu.SemaphoreType.DMA
    bf16 = jnp.bfloat16
    sides, tag_count = len(AROUND), up_to(fine.quads + coarse.quads, 16)
    fine_out, coarse_out = pl.pallas_call(
        functools.partial(kernel, fine, coarse, units, split),
        out_shape=[
            jax.ShapeDtypeStruct((fine.own, width), bf16),
            jax.ShapeDtypeStruct((coarse.lat_len, coarse.lon_len, wide_two), bf16),
        ],
        in_specs=[ANY] + [VMEM] * 10 + [ANY] * 5,
        out_specs=[ANY, VMEM],
        scratch_shapes=[pltpu.VMEM((fine.own, width), bf16)]
        + level_scratch(fine, width, heads)
        + [pltpu.VMEM((fine.own, width), bf16)]
        + level_scratch(coarse, wide_two, heads_two)
        + [pltpu.VMEM((coarse.quads * ROWS, wide_two), bf16)] * 2
        + [
            pltpu.VMEM((heads + heads_two, up_to(fine_table.shape[1], LANES)), jnp.float32),
            pltpu.VMEM((tag_count, LANES), bf16),
            pltpu.VMEM((sides, tag_count, LANES), bf16),
        ]
        + [pltpu.VMEM((lvls, w.shape[0], lons, w.shape[1], w.shape[2]), bf16) for w in weights]
        + [dma((2,)), dma((sides,)), dma((sides,))]
        + [dma((len(fine.halo),))] * 2
        + [dma((len(coarse.halo),))] * 2
        + gather_scratch(units, split),
        compiler_params=pltpu.CompilerParams(collective_id=1, has_side_effects=True, vmem_limit_bytes=LIMIT),
        name="levels",
    )(
        tokens.reshape(fine.own, width), fine_tags.reshape(lat_len, 1, lon_len),
        coarse_tags.reshape(coarse.lat_len, 1, coarse.lon_len), fine_gain[None], merge_gain[None], coarse_gain[None],
        fine_table, coarse_table, index, offset_numbers(), lane, *weights,
    )
    return fine_out.reshape(tokens.shape), coarse_out[None]


def solution(mesh):
    placed = (
        P(("grp", "lvl"), "lat", "lon", None),
        P(("grp", "lvl"), "lat", "lon"),
        P(("grp", "lvl"), "lat", "lon"),
        P(),
        P(None, "lon", "lvl"),
        P("lon", "lvl"),
        P(),
        P(),
        P("lon", "lvl"),
        P(),
        P(None, "lon", "lvl"),
        P("lon", "lvl"),
        P(),
    )
    return jax.shard_map(
        shards,
        mesh=mesh,
        in_specs=placed,
        out_specs=(P(("grp", "lvl"), "lat", "lon", None), P(("grp", "lvl"), "lat", "lon", None)),
        check_vma=False,
    )
```

```python
import functools
import math

import jax
import jax.numpy as jnp
import numpy as np
from jax import lax
from jax.experimental import pallas as pl
from jax.experimental.pallas import tpu as pltpu
from jax.sharding import PartitionSpec as P

WIN_LAT = 6
WIN_LON = 12
HALF_LAT = WIN_LAT // 2
HALF_LON = WIN_LON // 2
QUAD = HALF_LAT * HALF_LON
ROWS = -(-QUAD // 16) * 16
SENT = -(-QUAD // 8) * 8
WINDOW = 4 * ROWS
EPSILON = 1e-05
LANES = 128
LOG2E = math.log2(math.e)
MESH = pl.DeviceIdType.MESH
VMEM = pl.BlockSpec(memory_space=pltpu.VMEM)
ANY = pl.BlockSpec(memory_space=pl.ANY)
HBM = pl.BlockSpec(memory_space=pltpu.HBM)
LIMIT = 60 * 1024 * 1024
NT = (((1,), (1,)), ((), ()))
AROUND = ((0, -1), (0, 1), (-1, 0), (1, 0), (-1, -1), (-1, 1), (1, -1), (1, 1))
AHEAD = 3
LAG = 2
RELAYED = 3
ORDER = (2, 1, 3)
MERGE = 256
LAST = 256
SMALL = 10
FIRST = (32, 48)


def up_to(count, step):
    return -(-count // step) * step


class Plan:
    def __init__(self, lat_len, lon_len):
        self.lat_len, self.lon_len = lat_len, lon_len
        self.own = lat_len * lon_len
        self.down, self.across = lat_len // HALF_LAT, lon_len // HALF_LON
        self.quads = self.down * self.across
        self.columns = self.across // 2 + 1
        self.windows = (self.down // 2 + 1) * self.columns
        self.halo = []
        for side, (dy, dx) in enumerate(AROUND):
            rows = [-1] if dy < 0 else ([self.down] if dy > 0 else range(self.down))
            cols = [-1] if dx < 0 else ([self.across] if dx > 0 else range(self.across))
            for r in rows:
                for c in cols:
                    self.halo.append((side, r, c, (r % self.down) * self.across + c % self.across))

    def spot(self, r, c):
        window = ((r + 1) // 2) * self.columns + (c + 1) // 2
        return 4 * window + ((r + 1) % 2) * 2 + (c + 1) % 2

    def natural(self):
        result = np.full((self.quads * ROWS,), -1, np.int32)
        for q in range(self.quads):
            for p in range(QUAD):
                r = (q // self.across) * HALF_LAT + p // HALF_LON
                c = (q % self.across) * HALF_LON + p % HALF_LON
                result[q * ROWS + p] = r * self.lon_len + c
        return result

    def back(self, pitch):
        result = np.full((self.lat_len * pitch,), -1, np.int32)
        for row, token in enumerate(self.natural()):
            if token >= 0:
                result[token // self.lon_len * pitch + token % self.lon_len] = row
        return result

    def lanes(self):
        lane = np.arange(self.across * LANES)
        place = lane % ROWS
        column = (lane // LANES) * HALF_LON + place % HALF_LON
        return np.where(place < QUAD, column, -1), np.where(place < QUAD, place // HALF_LON, -1)


def patches(fine, coarse):
    token = coarse.natural()
    result = []
    for s in range(2):
        for t in range(2):
            a, b = token // coarse.lon_len, token % coarse.lon_len
            result.append(np.where(token >= 0, (2 * a + s) * fine.lon_len + 2 * b + t, -1))
    return np.concatenate(result)


def offset_numbers():
    spot = np.arange(WINDOW)
    place = spot % ROWS
    r = spot // ROWS // 2 * HALF_LAT + place // HALF_LON
    c = spot // ROWS % 2 * HALF_LON + place % HALF_LON
    number = (r[:, None] - r[None, :] + WIN_LAT - 1) * (2 * WIN_LON - 1) + c[:, None] - c[None, :] + WIN_LON - 1
    valid = (place < QUAD)[:, None] & (place < QUAD)[None, :]
    return np.where(valid, number, -1).astype(np.int32)


def onehot(index, width):
    spots = lax.broadcasted_iota(jnp.int32, (index.shape[0], width), 1)
    return jnp.where(spots == index, 1.0, 0.0).astype(jnp.bfloat16)


def pick(index, source):
    return jnp.dot(
        onehot(index, source.shape[0]), source, preferred_element_type=jnp.float32
    ).astype(jnp.bfloat16)


def normalize(values, gain):
    widened = values.astype(jnp.float32)
    center = widened - jnp.mean(widened, axis=-1, keepdims=True)
    spread = jnp.mean(center * center, axis=-1, keepdims=True)
    return (center * lax.rsqrt(spread + EPSILON) * gain).astype(jnp.bfloat16)


class Around:
    def __init__(self):
        self.lat, self.lon = lax.axis_index("lat"), lax.axis_index("lon")
        self.lats, self.lons = lax.axis_size("lat"), lax.axis_size("lon")

    def place(self, dy, dx):
        return {
            "lat": lax.rem(self.lat + dy + self.lats, self.lats),
            "lon": lax.rem(self.lon + dx + self.lons, self.lons),
        }

    def there(self, dy):
        return (self.lat > 0) if dy < 0 else (self.lat < self.lats - 1)

    def when_there(self, dy, action):
        if dy == 0:
            action()
        else:
            pl.when(self.there(dy))(action)

    def greet(self, barrier):
        for dy, dx in AROUND:
            def signal(dy=dy, dx=dx):
                pl.semaphore_signal(barrier, inc=1, device_id=self.place(dy, dx), device_id_type=MESH)
            self.when_there(dy, signal)
        return 2 + 3 * (self.lat > 0).astype(jnp.int32) + 3 * (self.lat < self.lats - 1).astype(jnp.int32)

    def copy(self, src, dst, send, recv, dy, dx):
        return pltpu.make_async_remote_copy(
            src_ref=src, dst_ref=dst, send_sem=send, recv_sem=recv,
            device_id=self.place(-dy, -dx), device_id_type=MESH,
        )


class Halo:
    def __init__(self, around, plan, own, wide, send, recv):
        self.around, self.plan, self.own, self.wide, self.send, self.recv = around, plan, own, wide, send, recv

    def copy(self, n):
        side, r, c, q = self.plan.halo[n]
        return self.around.copy(
            self.own.at[pl.ds(q * ROWS, SENT)], self.wide.at[pl.ds(self.plan.spot(r, c) * ROWS, SENT)],
            self.send.at[n], self.recv.at[n], *AROUND[side],
        )

    def clear(self):
        for _, r, c, _ in self.plan.halo:
            rows = pl.ds(self.plan.spot(r, c) * ROWS, ROWS)
            self.wide[rows, :] = jnp.zeros((ROWS, self.wide.shape[1]), self.wide.dtype)

    def start(self):
        for n, (side, *_) in enumerate(self.plan.halo):
            self.around.when_there(-AROUND[side][0], lambda n=n: self.copy(n).start())

    def finish(self):
        for n, (side, *_) in enumerate(self.plan.halo):
            self.around.when_there(AROUND[side][0], lambda n=n: self.copy(n).wait_recv())

    def drain(self):
        for n, (side, *_) in enumerate(self.plan.halo):
            self.around.when_there(-AROUND[side][0], lambda n=n: self.copy(n).wait_send())


class Gather:
    def __init__(self, shards, fulls, units, split, sems):
        self.shards, self.fulls, self.units, self.split, self.sems = shards, fulls, units, split, sems
        self.index = {a: lax.axis_index(a) for a in ("grp", "lat", "lon", "lvl")}
        self.size = {a: lax.axis_size(a) for a in ("grp", "lat", "lon", "lvl")}
        self.slots = range(1, self.size["lon"])
        self.plane = ("lat", "grp")
        self.line = split and self.size["lon"] == 4
        self.now = self.arrived = self.forwarded = self.shared = 0

    def at(self, axis, step):
        return {axis: lax.rem(self.index[axis] + step + self.size[axis], self.size[axis])}

    def greet(self, barrier):
        peers = 0
        for axis in ("lon", "lvl", "lat", "grp") if self.split else ("lon", "lvl"):
            for d in range(1, self.size[axis]):
                pl.semaphore_signal(barrier, inc=1, device_id=self.at(axis, d), device_id_type=MESH)
                peers += 1
        return peers

    def block_of(self, slot):
        return lax.rem(self.index["lon"] + slot, self.size["lon"]) if self.split else slot

    def rows(self, u):
        return self.shards[self.units[u][0]].shape[1]

    def piece(self, u, other=None):
        if not self.split:
            return 0, self.rows(u)
        size = self.rows(u) // 4
        lat, grp = [1 - self.index[a] if a == other else self.index[a] for a in self.plane]
        return pl.multiple_of((lat * 2 + grp) * size, 16), size

    def held(self, u, start, size):
        m, k, depth, col, cols = self.units[u]
        return self.shards[m].at[pl.ds(k, depth), pl.ds(start, size), pl.ds(col, cols)]

    def block(self, u, slot, slots, start, size):
        m, k, depth, col, cols = self.units[u]
        return self.fulls[m].at[
            self.index["lvl"], pl.ds(k, depth), pl.ds(slot, slots), pl.ds(start, size), pl.ds(col, cols)
        ]

    def slot(self, u, slot, start, size):
        m, k, depth, col, cols = self.units[u]
        return self.fulls[m].at[self.index["lvl"], pl.ds(k, depth), slot, pl.ds(start, size), pl.ds(col, cols)]

    def remote(self, src, dst, kind, number, device):
        send, recv = self.sems[1 + 2 * kind], self.sems[2 + 2 * kind]
        return pltpu.make_async_remote_copy(
            src_ref=src, dst_ref=dst, send_sem=send.at[number], recv_sem=recv.at[number],
            device_id=device, device_id_type=MESH,
        )

    def own_copy(self, u):
        slot = 0 if self.split else self.index["lon"]
        return pltpu.make_async_copy(
            self.held(u, 0, self.rows(u)), self.slot(u, slot, 0, self.rows(u)), self.sems[0].at[u]
        )

    def lon_copy(self, u, s):
        start, size = self.piece(u)
        slot = s if self.split else self.index["lon"]
        return self.remote(
            self.held(u, start, size), self.slot(u, slot, start, size), 0, (u, s - 1), self.at("lon", -s)
        )

    def near_copy(self, u, n):
        block = self.block(u, 1, self.size["lon"] - 1, *self.piece(u))
        return self.remote(block, block, 1, (u, n), self.at(self.plane[n], 1))

    def far_copy(self, u, n):
        start, size = self.piece(u, self.plane[n])
        cut = size * FIRST[u % len(FIRST)] // 64 // 16 * 16
        start, size = (start, cut) if n == 0 else (pl.multiple_of(start + cut, 16), size - cut)
        block = self.block(u, 1, self.size["lon"] - 1, start, size)
        return self.remote(block, block, 2, (u, n), self.at(self.plane[1 - n], 1))

    def lvl_copy(self, u):
        block = self.block(u, 0, self.size["lon"], 0, self.rows(u))
        return self.remote(block, block, 3, (u,), self.at("lvl", 1))

    def relayed(self, u):
        return self.line and RELAYED <= u < len(self.units)

    def direct(self, u, s, action):
        if s == 2 or not self.relayed(u):
            action()
        else:
            pl.when(self.index["lon"] > 0 if s == 1 else self.index["lon"] < 3)(action)

    def relays(self, u, action):
        for lon, slot, step in ((2, 1, 1), (1, 3, -1)) if self.relayed(u) else ():
            def act(slot=slot, step=step):
                place = self.piece(u)
                action(pltpu.make_async_remote_copy(
                    src_ref=self.slot(u, 2, *place), dst_ref=self.slot(u, slot, *place),
                    send_sem=self.sems[9].at[u], recv_sem=self.sems[2].at[u, slot - 1],
                    device_id=self.at("lon", step), device_id_type=MESH,
                ))
            pl.when(self.index["lon"] == lon)(act)

    def relay(self, u):
        if self.relayed(u):
            self.lon_copy(u, 2).wait_recv()
            self.relays(u, lambda copy: copy.start())

    def issue(self, u):
        if u < len(self.units):
            for s in ORDER if self.line else self.slots:
                self.direct(u, s, lambda s=s: self.lon_copy(u, s).start())
            self.own_copy(u).start()

    def begin(self):
        for u in range(AHEAD):
            self.issue(u)

    def arrive(self):
        u = self.arrived
        self.arrived += 1
        for s in self.slots:
            if s != 2 or not self.relayed(u):
                self.lon_copy(u, s).wait_recv()
        if self.split:
            for n in range(2):
                self.near_copy(u, n).start()
        self.issue(u + AHEAD)

    def forward(self):
        u = self.forwarded
        self.forwarded += 1
        if self.split:
            for n in range(2):
                self.near_copy(u, n).wait_recv()
                self.far_copy(u, n).start()

    def share(self):
        u = self.shared
        self.shared += 1
        if self.split:
            for n in range(2):
                self.far_copy(u, n).wait_recv()
        self.own_copy(u).wait()
        self.lvl_copy(u).start()

    def step(self, times=1):
        for _ in range(times):
            k, count = self.now, len(self.units)
            self.now += 1
            if k < count:
                self.arrive()
            if 0 <= k - LAG < count:
                self.forward()
            if 0 <= k - 2 * LAG < count:
                self.share()
            self.relay(k + 1)

    def ready(self, u):
        while self.shared <= u:
            self.step()
        self.lvl_copy(u).wait_recv()

    def end(self):
        for u in range(len(self.units)):
            self.lvl_copy(u).wait_send()
            for s in self.slots:
                self.direct(u, s, lambda s=s: self.lon_copy(u, s).wait_send())
            self.relays(u, lambda copy: copy.wait_send())
            if self.split:
                for n in range(2):
                    self.near_copy(u, n).wait_send()
                    self.far_copy(u, n).wait_send()


def weight_units(shards):
    fine_inward, fine_outward, merge, coarse_inward, coarse_outward = [s.shape for s in shards]
    units = [(0, k, 1, 0, fine_inward[2]) for k in range(3)]
    units.append((1, 0, 1, 0, fine_outward[2]))
    units += [(2, 0, 1, c, MERGE) for c in range(0, merge[2], MERGE)]
    units += [(3, 0, 3, c, LANES) for c in range(0, coarse_inward[2], LANES)]
    units += [(4, 0, 1, c, LAST) for c in range(0, coarse_outward[2], LAST)]
    return units


def gather_scratch(units):
    count, lons = len(units), lax.axis_size("lon")
    dma = pltpu.SemaphoreType.DMA
    return [dma((count,))] + [dma((count, lons - 1))] * 2 + [dma((count, 2))] * 4 + [dma((count,))] * 3


def flat(block):
    return block.reshape(block.shape[0] * block.shape[1], block.shape[2])


def turned(ref, rows, block_of, slots):
    size = ref.shape[1] // slots
    if size % LANES:
        return ref[rows, :]
    return jnp.concatenate(
        [ref[rows, pl.ds(pl.multiple_of(block_of(s) * size, size), size)] for s in range(slots)], axis=1
    )


def turn_back(value, block_of, slots, store):
    size = value.shape[1] // slots
    if size % LANES:
        store(slice(None), value)
        return
    for s in range(slots):
        store(pl.ds(pl.multiple_of(block_of(s) * size, size), size), value[:, s * size : (s + 1) * size])


def tag_rows(plan, tags_ref, column, place, features):
    grid = jnp.concatenate([tags_ref[r].astype(jnp.float32) for r in range(plan.lat_len)], axis=0)
    spots = lax.broadcasted_iota(jnp.int32, (plan.lon_len, features), 0)
    hot = jnp.where(spots == column, 1.0, 0.0).astype(jnp.bfloat16)
    spread = jnp.dot(grid.astype(jnp.bfloat16), hot, preferred_element_type=jnp.float32)
    rows = []
    for q in range(plan.down):
        row = jnp.zeros((1, features), jnp.float32)
        for k in range(HALF_LAT):
            r = q * HALF_LAT + k
            row = jnp.where(place == k, spread[r : r + 1, :], row)
        rows.append(row)
    return jnp.concatenate(
        [row[:, c * LANES : (c + 1) * LANES] for row in rows for c in range(plan.across)], axis=0
    )


def fill_masks(plan, tags, offset, masks):
    lane = lax.broadcasted_iota(jnp.int32, (ROWS, LANES), 1)
    row = lax.broadcasted_iota(jnp.int32, (ROWS, LANES), 0)
    owner = lax.broadcasted_iota(jnp.int32, (1, LANES), 1) // ROWS

    def tag_row(r, c):
        dy = -1 if r < 0 else int(r >= plan.down)
        dx = -1 if c < 0 else int(c >= plan.across)
        side = AROUND.index((dy, dx)) if dy or dx else len(AROUND)
        row = offset + r % plan.down * plan.across + c % plan.across
        return tags[side][row : row + 1]

    for q in range(plan.quads):
        r, c = divmod(q, plan.across)
        top, left = r - (r + 1) % 2, c - (c + 1) % 2
        across = tag_row(top, left)
        for a in range(1, 4):
            across = jnp.where(owner == a, tag_row(top + a // 2, left + a % 2), across)
        down = jnp.sum(jnp.where(lane == row, tag_row(r, c), 0.0), axis=-1, keepdims=True)
        masks[q] = jnp.where(down == across, 0.0, -1e30)


def split_table(tables, padded):
    padded[...] = jnp.zeros_like(padded)
    start = 0
    for table in tables:
        heads, entries = table.shape
        padded[start : start + heads, :entries] = table[...] * LOG2E
        start += heads
    rest, terms = padded[...], []
    for _ in range(3):
        term = rest.astype(jnp.bfloat16)
        terms.append(term)
        rest = rest - term.astype(jnp.float32)
    return jnp.concatenate(terms, axis=0)


def fill_bias(parts, number_ref, biases, first, last):
    total = parts.shape[0] // 3
    spots = lax.broadcasted_iota(jnp.int32, (parts.shape[1], LANES), 0)
    for p in range(first, last):
        row = p // QUAD * ROWS + p % QUAD
        hot = jnp.where(spots == number_ref[row : row + 1, :], 1.0, 0.0).astype(jnp.bfloat16)
        terms = jnp.dot(parts, hot, preferred_element_type=jnp.float32)
        value = terms[:total] + terms[total : 2 * total] + terms[2 * total :]
        start = 0
        for bias in biases:
            bias[:, row, :] = value[start : start + bias.shape[0]]
            start += bias.shape[0]


def attend(plan, spots, query, keys, values, bias_ref, masks, mixed, size):
    heads = LANES // size
    owner = lax.broadcasted_iota(jnp.int32, (ROWS, LANES), 1) // size
    ones = jnp.ones((WINDOW, LANES), jnp.bfloat16)
    where, scores, weights, both = [], [], [], []
    for q, group in spots:
        r = lax.div(q, plan.across)
        c = q - r * plan.across
        window = lax.div(r + 1, 2) * plan.columns + lax.div(c + 1, 2)
        place = lax.rem(r + 1, 2) * 2 + lax.rem(c + 1, 2)
        where.append((
            q, group, pl.ds(pl.multiple_of(q * ROWS, ROWS), ROWS), pl.ds(pl.multiple_of(window * WINDOW, WINDOW), WINDOW),
            pl.ds(pl.multiple_of(place * ROWS, ROWS), ROWS), slice(group * LANES, (group + 1) * LANES),
        ))
    for q, group, rows, others, inside, cols in where:
        block = query[rows, cols]
        stack = jnp.concatenate([jnp.where(owner == h, block, jnp.zeros_like(block)) for h in range(heads)], axis=0)
        scores.append(lax.dot_general(stack, keys[others, cols], NT, preferred_element_type=jnp.float32))
    for (q, group, rows, others, inside, cols), score in zip(where, scores):
        bias = bias_ref[group * heads : (group + 1) * heads, inside, :].reshape(heads * ROWS, LANES)
        score = score + bias + jnp.concatenate([masks[q]] * heads, axis=0)
        weights.append(jnp.exp2(score - jnp.max(score, axis=-1, keepdims=True)).astype(jnp.bfloat16))
    for (q, group, rows, others, inside, cols), weight in zip(where, weights):
        both.append(jnp.dot(
            weight, jnp.concatenate([values[others, cols], ones], axis=1), preferred_element_type=jnp.float32
        ))
    for (q, group, rows, others, inside, cols), part in zip(where, both):
        blended, totals = part[:ROWS, :LANES], part[:ROWS, LANES:]
        for h in range(1, heads):
            result = part[h * ROWS : (h + 1) * ROWS]
            blended = jnp.where(owner == h, result[:, :LANES], blended)
            totals = jnp.where(owner == h, result[:, LANES:], totals)
        mixed[rows, cols] = (blended / totals).astype(jnp.bfloat16)


def kernel(
    fine, coarse, units, split, tokens_ref, *refs,
):
    run(fine, coarse, units, split, tokens_ref, refs[:SMALL], *refs[SMALL:])


def run(
    fine, coarse, units, split, tokens_ref, small, s0, s1, s2, s3, s4, fine_ref, coarse_ref,
    fine_tags, coarse_tags, lane_ref, fine_gain, index_ref, fine_table, coarse_table, number_ref, merge_gain,
    coarse_gain, tokens, own, wide, query, keys, values, mixed, fine_bias, fine_masks, fine_value,
    two_own, two_wide, two_query, two_keys, two_values, two_mixed, coarse_bias, coarse_masks, two_in, two_value,
    padded, tag_own, tag_wide, f0, f1, f2, f3, f4, local, tag_send, tag_recv, send1, recv1, send2, recv2, *sems,
):
    width, wide_two = tokens.shape[1], two_own.shape[1]
    heads, heads_two = fine_bias.shape[0], coarse_bias.shape[0]
    size = width // heads
    scale = size ** (-0.5) * LOG2E
    around = Around()
    lons, lvls = lax.axis_size("lon"), lax.axis_size("lvl")
    gather = Gather((s0, s1, s2, s3, s4), (f0, f1, f2, f3, f4), units, split, sems)
    block_of = gather.block_of
    tag_wide[...] = jnp.zeros_like(tag_wide)
    halo = Halo(around, fine, own, wide, send1, recv1)
    halo_two = Halo(around, coarse, two_own, two_wide, send2, recv2)
    halo.clear()
    halo_two.clear()
    barrier = pltpu.get_barrier_semaphore()
    peers = around.greet(barrier) + gather.greet(barrier)
    brought = (
        fine_tags, coarse_tags, lane_ref, fine_gain, index_ref, fine_table, coarse_table, number_ref, merge_gain,
        coarse_gain,
    )
    fetches = [pltpu.make_async_copy(src, dst, local.at[2 + n]) for n, (src, dst) in enumerate(zip(small, brought))]
    for fetch in fetches[:3]:
        fetch.start()
    fetch = pltpu.make_async_copy(tokens_ref, tokens, local.at[0])
    fetch.start()
    for other in fetches[3:]:
        other.start()
    pl.semaphore_wait(barrier, peers)
    gather.begin()
    for other in fetches[:3]:
        other.wait()
    fine_lanes = fine.across * LANES
    coarse_lanes = coarse.across * LANES
    top = tag_rows(fine, fine_tags, lane_ref[0:1, :fine_lanes], lane_ref[1:2, :fine_lanes], fine_lanes)
    spare = jnp.zeros((tag_own.shape[0] - fine.quads - coarse.quads, LANES), jnp.float32)
    low = tag_rows(coarse, coarse_tags, lane_ref[0:1, fine_lanes:], lane_ref[1:2, fine_lanes:], coarse_lanes)
    tag_own[...] = jnp.concatenate([top, low, spare], axis=0).astype(jnp.bfloat16)

    def tag_copy(side):
        dy, dx = AROUND[side]
        return around.copy(tag_own, tag_wide.at[side], tag_send.at[side], tag_recv.at[side], dy, dx)

    for side, (dy, dx) in enumerate(AROUND):
        around.when_there(-dy, lambda side=side: tag_copy(side).start())

    fetch.wait()
    fetches[3].wait()
    fetches[4].wait()
    normed = normalize(tokens[...], fine_gain[...])
    arranged = pick(index_ref[: fine.quads * ROWS, 0:1], normed)
    own[...] = arranged
    halo.start()
    for q in range(fine.quads):
        spot = fine.spot(*divmod(q, fine.across))
        wide[pl.ds(spot * ROWS, ROWS), :] = arranged[q * ROWS : (q + 1) * ROWS]

    for other in fetches[5:]:
        other.wait()
    parts = split_table((fine_table, coarse_table), padded)
    fine_bias[...] = jnp.zeros_like(fine_bias)
    coarse_bias[...] = jnp.zeros_like(coarse_bias)
    chunk = 4 * QUAD // 6
    for first in range(0, 4 * QUAD, chunk):
        fill_bias(parts, number_ref, (fine_bias, coarse_bias), first, first + chunk)
        if first:
            gather.step()

    for side, (dy, dx) in enumerate(AROUND):
        around.when_there(dy, lambda side=side: tag_copy(side).wait_recv())
    tags = [tag_wide[side].astype(jnp.float32) for side in range(len(AROUND))] + [tag_own[...].astype(jnp.float32)]
    fill_masks(fine, tags, 0, fine_masks)
    fill_masks(coarse, tags, fine.quads, coarse_masks)

    gather.ready(0)
    half = width // lvls
    for lvl in range(lvls):
        part = jnp.dot(turned(own, slice(None), block_of, lons), flat(f0[lvl, 0]), preferred_element_type=jnp.float32)
        query[:, lvl * half : (lvl + 1) * half] = (part * scale).astype(jnp.bfloat16)
    halo.finish()
    for member, target in ((1, keys), (2, values)):
        gather.ready(member)

        @pl.loop(0, fine.windows // fine.columns)
        def _(band):
            count = fine.columns * WINDOW
            rows = pl.ds(pl.multiple_of(band * count, count), count)
            x = turned(wide, rows, block_of, lons)
            for lvl in range(lvls):
                part = jnp.dot(x, flat(f0[lvl, member]), preferred_element_type=jnp.float32)
                target[rows, lvl * half : (lvl + 1) * half] = part.astype(jnp.bfloat16)

    per_row = fine.across
    for first in range(0, fine.quads, per_row):
        @pl.loop(first, first + per_row, step=2)
        def _(q):
            attend(
                fine, [(q + i, group) for i in range(2) for group in range(width // LANES)], query, keys, values,
                fine_bias, fine_masks, mixed, size,
            )
        gather.step()

    own_mixed = pick(index_ref[: fine.own, 1:2], mixed[...])
    gather.ready(3)
    update = None
    for lvl in range(lvls):
        term = lax.dot_general(
            own_mixed[:, lvl * half : (lvl + 1) * half], flat(f1[lvl, 0]), NT, preferred_element_type=jnp.float32
        )
        update = term if update is None else update + term

    def put_fine(cols, value):
        fine_value[:, cols] = (tokens[:, cols].astype(jnp.float32) + value).astype(jnp.bfloat16)

    turn_back(update, block_of, lons, put_fine)
    publish = pltpu.make_async_copy(fine_value, fine_ref, local.at[1])
    publish.start()

    count = coarse.quads * ROWS
    stacked = pick(index_ref[: 4 * count, 2:3], fine_value[...]).astype(jnp.float32)
    members = [stacked[m * count : (m + 1) * count] for m in range(4)]
    mean = sum(jnp.sum(m, axis=-1, keepdims=True) for m in members) / (4 * width)
    centers = [m - mean for m in members]
    spread = sum(jnp.sum(c * c, axis=-1, keepdims=True) for c in centers) / (4 * width)
    factor = lax.rsqrt(spread + EPSILON)
    normed = jnp.concatenate(
        [(centers[m] * factor * merge_gain[:, m * width : (m + 1) * width]).astype(jnp.bfloat16) for m in range(4)],
        axis=1,
    )
    merged = None
    share = 4 * width // lvls
    for u in [u for u in range(len(units)) if units[u][0] == 2]:
        gather.ready(u)
        _, _, _, col, cols = units[u]
        for lvl in range(lvls):
            start = lvl * share + col
            term = lax.dot_general(
                normed[:, start : start + cols], flat(f2[lvl, 0, :, :, col : col + cols]), NT,
                preferred_element_type=jnp.float32,
            )
            merged = term if merged is None else merged + term

    def put_coarse(cols, value):
        two_in[:, cols] = value.astype(jnp.bfloat16)

    turn_back(merged, block_of, lons, put_coarse)
    two_own[...] = normalize(two_in[...], coarse_gain[...])
    halo_two.start()
    for q in range(coarse.quads):
        spot = coarse.spot(*divmod(q, coarse.across))
        two_wide[pl.ds(spot * ROWS, ROWS), :] = two_own[q * ROWS : (q + 1) * ROWS, :]
    gather.step(2)
    halo_two.finish()

    share = wide_two // lvls
    inner = [u for u in range(len(units)) if units[u][0] == 3]
    for u in inner:
        gather.ready(u)
        _, _, _, col, cols = units[u]
        for lvl in range(lvls):
            start = lvl * share + col
            part = jnp.dot(
                turned(two_own, slice(None), block_of, lons), flat(f3[lvl, 0, :, :, col : col + cols]),
                preferred_element_type=jnp.float32,
            )
            two_query[:, start : start + cols] = (part * scale).astype(jnp.bfloat16)
            weight = jnp.concatenate([flat(f3[lvl, k, :, :, col : col + cols]) for k in (1, 2)], axis=1)
            part = jnp.dot(
                turned(two_wide, slice(None), block_of, lons), weight, preferred_element_type=jnp.float32
            ).astype(jnp.bfloat16)
            two_keys[:, start : start + cols] = part[:, :cols]
            two_values[:, start : start + cols] = part[:, cols:]

        attend(
            coarse, [(q, (lvl * share + col) // LANES) for q in range(coarse.quads) for lvl in range(lvls)],
            two_query, two_keys, two_values, coarse_bias, coarse_masks, two_mixed, size,
        )

    update = None
    for u in [u for u in range(len(units)) if units[u][0] == 4]:
        gather.ready(u)
        _, _, _, col, cols = units[u]
        for lvl in range(lvls):
            start = lvl * share + col
            term = lax.dot_general(
                two_mixed[:, start : start + cols], flat(f4[lvl, 0, :, :, col : col + cols]), NT,
                preferred_element_type=jnp.float32,
            )
            update = term if update is None else update + term

    def put_out(cols, value):
        two_value[:, cols] = (two_in[:, cols].astype(jnp.float32) + value).astype(jnp.bfloat16)

    turn_back(update, block_of, lons, put_out)
    pitch = up_to(coarse.lon_len, 16)
    result = pick(index_ref[: coarse.lat_len * pitch, 3:4], two_value[...])
    for r in range(coarse.lat_len):
        coarse_ref[r] = result[r * pitch : r * pitch + coarse.lon_len]

    publish.wait()
    gather.end()
    for side, (dy, dx) in enumerate(AROUND):
        around.when_there(-dy, lambda side=side: tag_copy(side).wait_send())
    halo.drain()
    halo_two.drain()


def level_scratch(plan, features, heads):
    rows, all_rows = plan.quads * ROWS, plan.windows * WINDOW
    return [
        pltpu.VMEM((rows, features), jnp.bfloat16),
        pltpu.VMEM((all_rows, features), jnp.bfloat16),
        pltpu.VMEM((rows, features), jnp.bfloat16),
        pltpu.VMEM((all_rows, features), jnp.bfloat16),
        pltpu.VMEM((all_rows, features), jnp.bfloat16),
        pltpu.VMEM((rows, features), jnp.bfloat16),
        pltpu.VMEM((heads, WINDOW, LANES), jnp.float32),
        pltpu.VMEM((plan.quads, ROWS, LANES), jnp.float32),
    ]


def shards(
    tokens, fine_tags, coarse_tags, fine_gain, fine_inward, fine_outward, fine_table, merge_gain,
    merge_weight, coarse_gain, coarse_inward, coarse_outward, coarse_table,
):
    _, lat_len, lon_len, width = tokens.shape
    fine, coarse = Plan(lat_len, lon_len), Plan(lat_len // 2, lon_len // 2)
    weights = [fine_inward, fine_outward[None], merge_weight[None], coarse_inward, coarse_outward[None]]
    grps, lats, lons, lvls = (lax.axis_size(a) for a in ("grp", "lat", "lon", "lvl"))
    split = grps == 2 and lats == 2 and all(w.shape[1] % LANES == 0 for w in weights)
    units = weight_units(weights)
    wide_two = coarse_inward.shape[1] * lons
    heads, heads_two = fine_table.shape[0], coarse_table.shape[0]
    pitch = up_to(coarse.lon_len, 16)

    columns = [fine.natural(), fine.back(fine.lon_len), patches(fine, coarse), coarse.back(pitch)]
    index = np.full((max(len(c) for c in columns), len(columns)), -1, np.int32)
    for n, column in enumerate(columns):
        index[: len(column), n] = column
    lane = np.concatenate([np.stack(p.lanes()) for p in (fine, coarse)], axis=1).astype(np.int32)

    small = [
        fine_tags.reshape(lat_len, 1, lon_len), coarse_tags.reshape(coarse.lat_len, 1, coarse.lon_len), lane,
        fine_gain[None], index, fine_table, coarse_table, offset_numbers(), merge_gain[None], coarse_gain[None],
    ]
    dma = pltpu.SemaphoreType.DMA
    bf16 = jnp.bfloat16
    sides, tag_count = len(AROUND), up_to(fine.quads + coarse.quads, 16)
    fine_out, coarse_out = pl.pallas_call(
        functools.partial(kernel, fine, coarse, units, split),
        out_shape=[
            jax.ShapeDtypeStruct((fine.own, width), bf16),
            jax.ShapeDtypeStruct((coarse.lat_len, coarse.lon_len, wide_two), bf16),
        ],
        in_specs=[HBM] * (1 + SMALL + len(weights)),
        out_specs=[ANY, VMEM],
        scratch_shapes=[pltpu.VMEM(x.shape, x.dtype) for x in small]
        + [pltpu.VMEM((fine.own, width), bf16)]
        + level_scratch(fine, width, heads)
        + [pltpu.VMEM((fine.own, width), bf16)]
        + level_scratch(coarse, wide_two, heads_two)
        + [pltpu.VMEM((coarse.quads * ROWS, wide_two), bf16)] * 2
        + [
            pltpu.VMEM((heads + heads_two, up_to(fine_table.shape[1], LANES)), jnp.float32),
            pltpu.VMEM((tag_count, LANES), bf16),
            pltpu.VMEM((sides, tag_count, LANES), bf16),
        ]
        + [pltpu.VMEM((lvls, w.shape[0], lons, w.shape[1], w.shape[2]), bf16) for w in weights]
        + [dma((2 + SMALL,)), dma((sides,)), dma((sides,))]
        + [dma((len(fine.halo),))] * 2
        + [dma((len(coarse.halo),))] * 2
        + gather_scratch(units),
        compiler_params=pltpu.CompilerParams(collective_id=1, has_side_effects=True, vmem_limit_bytes=LIMIT),
        name="levels",
    )(
        tokens.reshape(fine.own, width), *small, *weights,
    )
    return fine_out.reshape(tokens.shape), coarse_out[None]


def solution(mesh):
    placed = (
        P(("grp", "lvl"), "lat", "lon", None),
        P(("grp", "lvl"), "lat", "lon"),
        P(("grp", "lvl"), "lat", "lon"),
        P(),
        P(None, "lon", "lvl"),
        P("lon", "lvl"),
        P(),
        P(),
        P("lon", "lvl"),
        P(),
        P(None, "lon", "lvl"),
        P("lon", "lvl"),
        P(),
    )
    return jax.shard_map(
        shards,
        mesh=mesh,
        in_specs=placed,
        out_specs=(P(("grp", "lvl"), "lat", "lon", None), P(("grp", "lvl"), "lat", "lon", None)),
        check_vma=False,
    )
```

```python
import functools
import math

import jax
import jax.numpy as jnp
import numpy as np
from jax import lax
from jax.experimental import pallas as pl
from jax.experimental.pallas import tpu as pltpu
from jax.sharding import PartitionSpec as P

WIN_LAT = 6
WIN_LON = 12
HALF_LAT = WIN_LAT // 2
HALF_LON = WIN_LON // 2
QUAD = HALF_LAT * HALF_LON
ROWS = -(-QUAD // 16) * 16
SENT = -(-QUAD // 8) * 8
WINDOW = 4 * ROWS
EPSILON = 1e-05
LANES = 128
LOG2E = math.log2(math.e)
MESH = pl.DeviceIdType.MESH
VMEM = pl.BlockSpec(memory_space=pltpu.VMEM)
ANY = pl.BlockSpec(memory_space=pl.ANY)
HBM = pl.BlockSpec(memory_space=pltpu.HBM)
LIMIT = 60 * 1024 * 1024
NT = (((1,), (1,)), ((), ()))
AROUND = ((0, -1), (0, 1), (-1, 0), (1, 0), (-1, -1), (-1, 1), (1, -1), (1, 1))
AHEAD = 3
LAG = 2
RELAYED = 3
ORDER = (1, 3, 2)
MERGE = 256
LAST = 256
SMALL = 10
FIRST = (32, 48)


def up_to(count, step):
    return -(-count // step) * step


class Plan:
    def __init__(self, lat_len, lon_len):
        self.lat_len, self.lon_len = lat_len, lon_len
        self.own = lat_len * lon_len
        self.down, self.across = lat_len // HALF_LAT, lon_len // HALF_LON
        self.quads = self.down * self.across
        self.columns = self.across // 2 + 1
        self.windows = (self.down // 2 + 1) * self.columns
        self.halo = []
        for side, (dy, dx) in enumerate(AROUND):
            rows = [-1] if dy < 0 else ([self.down] if dy > 0 else range(self.down))
            cols = [-1] if dx < 0 else ([self.across] if dx > 0 else range(self.across))
            for r in rows:
                for c in cols:
                    self.halo.append((side, r, c, (r % self.down) * self.across + c % self.across))

    def spot(self, r, c):
        window = ((r + 1) // 2) * self.columns + (c + 1) // 2
        return 4 * window + ((r + 1) % 2) * 2 + (c + 1) % 2

    def natural(self):
        result = np.full((self.quads * ROWS,), -1, np.int32)
        for q in range(self.quads):
            for p in range(QUAD):
                r = (q // self.across) * HALF_LAT + p // HALF_LON
                c = (q % self.across) * HALF_LON + p % HALF_LON
                result[q * ROWS + p] = r * self.lon_len + c
        return result

    def back(self, pitch):
        result = np.full((self.lat_len * pitch,), -1, np.int32)
        for row, token in enumerate(self.natural()):
            if token >= 0:
                result[token // self.lon_len * pitch + token % self.lon_len] = row
        return result

    def lanes(self):
        lane = np.arange(self.across * LANES)
        place = lane % ROWS
        column = (lane // LANES) * HALF_LON + place % HALF_LON
        return np.where(place < QUAD, column, -1), np.where(place < QUAD, place // HALF_LON, -1)


def patches(fine, coarse):
    token = coarse.natural()
    result = []
    for s in range(2):
        for t in range(2):
            a, b = token // coarse.lon_len, token % coarse.lon_len
            result.append(np.where(token >= 0, (2 * a + s) * fine.lon_len + 2 * b + t, -1))
    return np.concatenate(result)


def offset_numbers():
    spot = np.arange(WINDOW)
    place = spot % ROWS
    r = spot // ROWS // 2 * HALF_LAT + place // HALF_LON
    c = spot // ROWS % 2 * HALF_LON + place % HALF_LON
    number = (r[:, None] - r[None, :] + WIN_LAT - 1) * (2 * WIN_LON - 1) + c[:, None] - c[None, :] + WIN_LON - 1
    valid = (place < QUAD)[:, None] & (place < QUAD)[None, :]
    return np.where(valid, number, -1).astype(np.int32)


def onehot(index, width):
    spots = lax.broadcasted_iota(jnp.int32, (index.shape[0], width), 1)
    return jnp.where(spots == index, 1.0, 0.0).astype(jnp.bfloat16)


def pick(index, source):
    return jnp.dot(
        onehot(index, source.shape[0]), source, preferred_element_type=jnp.float32
    ).astype(jnp.bfloat16)


def normalize(values, gain):
    widened = values.astype(jnp.float32)
    center = widened - jnp.mean(widened, axis=-1, keepdims=True)
    spread = jnp.mean(center * center, axis=-1, keepdims=True)
    return (center * lax.rsqrt(spread + EPSILON) * gain).astype(jnp.bfloat16)


class Around:
    def __init__(self):
        self.lat, self.lon = lax.axis_index("lat"), lax.axis_index("lon")
        self.lats, self.lons = lax.axis_size("lat"), lax.axis_size("lon")

    def place(self, dy, dx):
        return {
            "lat": lax.rem(self.lat + dy + self.lats, self.lats),
            "lon": lax.rem(self.lon + dx + self.lons, self.lons),
        }

    def there(self, dy):
        return (self.lat > 0) if dy < 0 else (self.lat < self.lats - 1)

    def when_there(self, dy, action):
        if dy == 0:
            action()
        else:
            pl.when(self.there(dy))(action)

    def greet(self, barrier):
        for dy, dx in AROUND:
            def signal(dy=dy, dx=dx):
                pl.semaphore_signal(barrier, inc=1, device_id=self.place(dy, dx), device_id_type=MESH)
            self.when_there(dy, signal)
        return 2 + 3 * (self.lat > 0).astype(jnp.int32) + 3 * (self.lat < self.lats - 1).astype(jnp.int32)

    def copy(self, src, dst, send, recv, dy, dx):
        return pltpu.make_async_remote_copy(
            src_ref=src, dst_ref=dst, send_sem=send, recv_sem=recv,
            device_id=self.place(-dy, -dx), device_id_type=MESH,
        )


class Halo:
    def __init__(self, around, plan, own, wide, send, recv):
        self.around, self.plan, self.own, self.wide, self.send, self.recv = around, plan, own, wide, send, recv

    def copy(self, n):
        side, r, c, q = self.plan.halo[n]
        return self.around.copy(
            self.own.at[pl.ds(q * ROWS, SENT)], self.wide.at[pl.ds(self.plan.spot(r, c) * ROWS, SENT)],
            self.send.at[n], self.recv.at[n], *AROUND[side],
        )

    def clear(self):
        for side, r, c, _ in self.plan.halo:
            start, dy = self.plan.spot(r, c) * ROWS, AROUND[side][0]
            if SENT < ROWS:
                spare = pl.ds(start + SENT, ROWS - SENT)
                self.wide[spare, :] = jnp.zeros((ROWS - SENT, self.wide.shape[1]), self.wide.dtype)
            if dy:
                def beyond(start=start):
                    self.wide[pl.ds(start, SENT), :] = jnp.zeros((SENT, self.wide.shape[1]), self.wide.dtype)
                pl.when(jnp.logical_not(self.around.there(dy)))(beyond)

    def start(self):
        for n, (side, *_) in enumerate(self.plan.halo):
            self.around.when_there(-AROUND[side][0], lambda n=n: self.copy(n).start())

    def finish(self):
        for n, (side, *_) in enumerate(self.plan.halo):
            self.around.when_there(AROUND[side][0], lambda n=n: self.copy(n).wait_recv())

    def drain(self):
        for n, (side, *_) in enumerate(self.plan.halo):
            self.around.when_there(-AROUND[side][0], lambda n=n: self.copy(n).wait_send())


class Gather:
    def __init__(self, shards, fulls, units, split, sems):
        self.shards, self.fulls, self.units, self.split, self.sems = shards, fulls, units, split, sems
        self.index = {a: lax.axis_index(a) for a in ("grp", "lat", "lon", "lvl")}
        self.size = {a: lax.axis_size(a) for a in ("grp", "lat", "lon", "lvl")}
        self.slots = range(1, self.size["lon"])
        self.plane = ("lat", "grp")
        self.line = split and self.size["lon"] == 4
        self.now = self.arrived = self.forwarded = self.shared = 0

    def at(self, axis, step):
        return {axis: lax.rem(self.index[axis] + step + self.size[axis], self.size[axis])}

    def greet(self, barrier):
        peers = 0
        for axis in ("lon", "lvl", "lat", "grp") if self.split else ("lon", "lvl"):
            for d in range(1, self.size[axis]):
                pl.semaphore_signal(barrier, inc=1, device_id=self.at(axis, d), device_id_type=MESH)
                peers += 1
        return peers

    def block_of(self, slot):
        return lax.rem(self.index["lon"] + slot, self.size["lon"]) if self.split else slot

    def rows(self, u):
        return self.shards[self.units[u][0]].shape[1]

    def piece(self, u, other=None):
        if not self.split:
            return 0, self.rows(u)
        size = self.rows(u) // 4
        lat, grp = [1 - self.index[a] if a == other else self.index[a] for a in self.plane]
        return pl.multiple_of((lat * 2 + grp) * size, 16), size

    def held(self, u, start, size):
        m, k, depth, col, cols = self.units[u]
        return self.shards[m].at[pl.ds(k, depth), pl.ds(start, size), pl.ds(col, cols)]

    def block(self, u, slot, slots, start, size):
        m, k, depth, col, cols = self.units[u]
        return self.fulls[m].at[
            self.index["lvl"], pl.ds(k, depth), pl.ds(slot, slots), pl.ds(start, size), pl.ds(col, cols)
        ]

    def slot(self, u, slot, start, size):
        m, k, depth, col, cols = self.units[u]
        return self.fulls[m].at[self.index["lvl"], pl.ds(k, depth), slot, pl.ds(start, size), pl.ds(col, cols)]

    def remote(self, src, dst, kind, number, device):
        send, recv = self.sems[1 + 2 * kind], self.sems[2 + 2 * kind]
        return pltpu.make_async_remote_copy(
            src_ref=src, dst_ref=dst, send_sem=send.at[number], recv_sem=recv.at[number],
            device_id=device, device_id_type=MESH,
        )

    def own_copy(self, u):
        slot = 0 if self.split else self.index["lon"]
        return pltpu.make_async_copy(
            self.held(u, 0, self.rows(u)), self.slot(u, slot, 0, self.rows(u)), self.sems[0].at[u]
        )

    def lon_copy(self, u, s):
        start, size = self.piece(u)
        slot = s if self.split else self.index["lon"]
        return self.remote(
            self.held(u, start, size), self.slot(u, slot, start, size), 0, (u, s - 1), self.at("lon", -s)
        )

    def near_copy(self, u, n):
        block = self.block(u, 1, self.size["lon"] - 1, *self.piece(u))
        return self.remote(block, block, 1, (u, n), self.at(self.plane[n], 1))

    def far_copy(self, u, n):
        start, size = self.piece(u, self.plane[n])
        cut = size * FIRST[u % len(FIRST)] // 64 // 16 * 16
        start, size = (start, cut) if n == 0 else (pl.multiple_of(start + cut, 16), size - cut)
        block = self.block(u, 1, self.size["lon"] - 1, start, size)
        return self.remote(block, block, 2, (u, n), self.at(self.plane[1 - n], 1))

    def lvl_copy(self, u):
        block = self.block(u, 0, self.size["lon"], 0, self.rows(u))
        return self.remote(block, block, 3, (u,), self.at("lvl", 1))

    def relayed(self, u):
        return self.line and RELAYED <= u < len(self.units)

    def direct(self, u, s, action):
        if s == 2 or not self.relayed(u):
            action()
        else:
            pl.when(self.index["lon"] > 0 if s == 1 else self.index["lon"] < 3)(action)

    def relays(self, u, action):
        for lon, slot, step in ((2, 1, 1), (1, 3, -1)) if self.relayed(u) else ():
            def act(slot=slot, step=step):
                place = self.piece(u)
                action(pltpu.make_async_remote_copy(
                    src_ref=self.slot(u, 2, *place), dst_ref=self.slot(u, slot, *place),
                    send_sem=self.sems[9].at[u], recv_sem=self.sems[2].at[u, slot - 1],
                    device_id=self.at("lon", step), device_id_type=MESH,
                ))
            pl.when(self.index["lon"] == lon)(act)

    def relay(self, u):
        if self.relayed(u):
            self.lon_copy(u, 2).wait_recv()
            self.relays(u, lambda copy: copy.start())

    def issue(self, u):
        if u < len(self.units):
            for s in ORDER if self.line else self.slots:
                self.direct(u, s, lambda s=s: self.lon_copy(u, s).start())
            self.own_copy(u).start()

    def begin(self):
        for u in range(AHEAD):
            self.issue(u)

    def arrive(self):
        u = self.arrived
        self.arrived += 1
        for s in self.slots:
            if s != 2 or not self.relayed(u):
                self.lon_copy(u, s).wait_recv()
        if self.split:
            for n in range(2):
                self.near_copy(u, n).start()
        self.issue(u + AHEAD)

    def forward(self):
        u = self.forwarded
        self.forwarded += 1
        if self.split:
            for n in range(2):
                self.near_copy(u, n).wait_recv()
                self.far_copy(u, n).start()

    def share(self):
        u = self.shared
        self.shared += 1
        if self.split:
            for n in range(2):
                self.far_copy(u, n).wait_recv()
        self.own_copy(u).wait()
        self.lvl_copy(u).start()

    def step(self, times=1):
        for _ in range(times):
            k, count = self.now, len(self.units)
            self.now += 1
            if 0 <= k - LAG < count:
                self.forward()
            if 0 <= k - 2 * LAG < count:
                self.share()
            if k < count:
                self.arrive()
            self.relay(k + 1)

    def ready(self, u):
        while self.shared <= u:
            self.step()
        self.lvl_copy(u).wait_recv()

    def end(self):
        for u in range(len(self.units)):
            self.lvl_copy(u).wait_send()
            for s in self.slots:
                self.direct(u, s, lambda s=s: self.lon_copy(u, s).wait_send())
            self.relays(u, lambda copy: copy.wait_send())
            if self.split:
                for n in range(2):
                    self.near_copy(u, n).wait_send()
                    self.far_copy(u, n).wait_send()


def weight_units(shards):
    fine_inward, fine_outward, merge, coarse_inward, coarse_outward = [s.shape for s in shards]
    units = [(0, k, 1, 0, fine_inward[2]) for k in range(3)]
    units.append((1, 0, 1, 0, fine_outward[2]))
    units += [(2, 0, 1, c, MERGE) for c in range(0, merge[2], MERGE)]
    units += [(3, 0, 3, c, LANES) for c in range(0, coarse_inward[2], LANES)]
    units += [(4, 0, 1, c, LAST) for c in range(0, coarse_outward[2], LAST)]
    return units


def gather_scratch(units):
    count, lons = len(units), lax.axis_size("lon")
    dma = pltpu.SemaphoreType.DMA
    return [dma((count,))] + [dma((count, lons - 1))] * 2 + [dma((count, 2))] * 4 + [dma((count,))] * 3


def flat(block):
    return block.reshape(block.shape[0] * block.shape[1], block.shape[2])


def turned(ref, rows, block_of, slots):
    size = ref.shape[1] // slots
    if size % LANES:
        return ref[rows, :]
    return jnp.concatenate(
        [ref[rows, pl.ds(pl.multiple_of(block_of(s) * size, size), size)] for s in range(slots)], axis=1
    )


def turn_back(value, block_of, slots, store):
    size = value.shape[1] // slots
    if size % LANES:
        store(slice(None), value)
        return
    for s in range(slots):
        store(pl.ds(pl.multiple_of(block_of(s) * size, size), size), value[:, s * size : (s + 1) * size])


def tag_rows(plan, tags_ref, column, place, features):
    grid = jnp.concatenate([tags_ref[r].astype(jnp.float32) for r in range(plan.lat_len)], axis=0)
    spots = lax.broadcasted_iota(jnp.int32, (plan.lon_len, features), 0)
    hot = jnp.where(spots == column, 1.0, 0.0).astype(jnp.bfloat16)
    spread = jnp.dot(grid.astype(jnp.bfloat16), hot, preferred_element_type=jnp.float32)
    rows = []
    for q in range(plan.down):
        row = jnp.zeros((1, features), jnp.float32)
        for k in range(HALF_LAT):
            r = q * HALF_LAT + k
            row = jnp.where(place == k, spread[r : r + 1, :], row)
        rows.append(row)
    return jnp.concatenate(
        [row[:, c * LANES : (c + 1) * LANES] for row in rows for c in range(plan.across)], axis=0
    )


def fill_masks(plan, tags, offset, masks):
    lane = lax.broadcasted_iota(jnp.int32, (ROWS, LANES), 1)
    row = lax.broadcasted_iota(jnp.int32, (ROWS, LANES), 0)
    owner = lax.broadcasted_iota(jnp.int32, (1, LANES), 1) // ROWS

    def tag_row(r, c):
        dy = -1 if r < 0 else int(r >= plan.down)
        dx = -1 if c < 0 else int(c >= plan.across)
        side = AROUND.index((dy, dx)) if dy or dx else len(AROUND)
        row = offset + r % plan.down * plan.across + c % plan.across
        return tags[side][row : row + 1]

    for q in range(plan.quads):
        r, c = divmod(q, plan.across)
        top, left = r - (r + 1) % 2, c - (c + 1) % 2
        across = tag_row(top, left)
        for a in range(1, 4):
            across = jnp.where(owner == a, tag_row(top + a // 2, left + a % 2), across)
        down = jnp.sum(jnp.where(lane == row, tag_row(r, c), 0.0), axis=-1, keepdims=True)
        masks[q] = jnp.where(down == across, 0.0, -1e30)


def split_table(tables, padded):
    padded[...] = jnp.zeros_like(padded)
    start = 0
    for table in tables:
        heads, entries = table.shape
        padded[start : start + heads, :entries] = table[...] * LOG2E
        start += heads
    rest, terms = padded[...], []
    for _ in range(3):
        term = rest.astype(jnp.bfloat16)
        terms.append(term)
        rest = rest - term.astype(jnp.float32)
    return jnp.concatenate(terms, axis=0)


def fill_bias(parts, number_ref, biases, first, last):
    total = parts.shape[0] // 3
    spots = lax.broadcasted_iota(jnp.int32, (parts.shape[1], LANES), 0)
    for p in range(first, last):
        row = p // QUAD * ROWS + p % QUAD
        hot = jnp.where(spots == number_ref[row : row + 1, :], 1.0, 0.0).astype(jnp.bfloat16)
        terms = jnp.dot(parts, hot, preferred_element_type=jnp.float32)
        value = terms[:total] + terms[total : 2 * total] + terms[2 * total :]
        start = 0
        for bias in biases:
            bias[:, row, :] = value[start : start + bias.shape[0]]
            start += bias.shape[0]


def attend(plan, spots, query, keys, values, bias_ref, masks, mixed, size):
    heads = LANES // size
    owner = lax.broadcasted_iota(jnp.int32, (ROWS, LANES), 1) // size
    ones = jnp.ones((WINDOW, LANES), jnp.bfloat16)
    where, scores, weights, both = [], [], [], []
    for q, group in spots:
        r = lax.div(q, plan.across)
        c = q - r * plan.across
        window = lax.div(r + 1, 2) * plan.columns + lax.div(c + 1, 2)
        place = lax.rem(r + 1, 2) * 2 + lax.rem(c + 1, 2)
        where.append((
            q, group, pl.ds(pl.multiple_of(q * ROWS, ROWS), ROWS), pl.ds(pl.multiple_of(window * WINDOW, WINDOW), WINDOW),
            pl.ds(pl.multiple_of(place * ROWS, ROWS), ROWS), slice(group * LANES, (group + 1) * LANES),
        ))
    for q, group, rows, others, inside, cols in where:
        block = query[rows, cols]
        stack = jnp.concatenate([jnp.where(owner == h, block, jnp.zeros_like(block)) for h in range(heads)], axis=0)
        scores.append(lax.dot_general(stack, keys[others, cols], NT, preferred_element_type=jnp.float32))
    for (q, group, rows, others, inside, cols), score in zip(where, scores):
        bias = bias_ref[group * heads : (group + 1) * heads, inside, :].reshape(heads * ROWS, LANES)
        score = score + bias + jnp.concatenate([masks[q]] * heads, axis=0)
        weights.append(jnp.exp2(score - jnp.max(score, axis=-1, keepdims=True)).astype(jnp.bfloat16))
    for (q, group, rows, others, inside, cols), weight in zip(where, weights):
        both.append(jnp.dot(
            weight, jnp.concatenate([values[others, cols], ones], axis=1), preferred_element_type=jnp.float32
        ))
    for (q, group, rows, others, inside, cols), part in zip(where, both):
        blended, totals = part[:ROWS, :LANES], part[:ROWS, LANES:]
        for h in range(1, heads):
            result = part[h * ROWS : (h + 1) * ROWS]
            blended = jnp.where(owner == h, result[:, :LANES], blended)
            totals = jnp.where(owner == h, result[:, LANES:], totals)
        mixed[rows, cols] = (blended / totals).astype(jnp.bfloat16)


def kernel(
    fine, coarse, units, split, tokens_ref, *refs,
):
    run(fine, coarse, units, split, tokens_ref, refs[:SMALL], *refs[SMALL:])


def run(
    fine, coarse, units, split, tokens_ref, small, s0, s1, s2, s3, s4, fine_ref, coarse_ref,
    fine_tags, coarse_tags, lane_ref, fine_gain, index_ref, fine_table, coarse_table, number_ref, merge_gain,
    coarse_gain, tokens, own, wide, query, keys, values, mixed, fine_bias, fine_masks, fine_value,
    two_own, two_wide, two_query, two_keys, two_values, two_mixed, coarse_bias, coarse_masks, two_in, two_value,
    padded, tag_own, tag_wide, f0, f1, f2, f3, f4, local, tag_send, tag_recv, send1, recv1, send2, recv2, *sems,
):
    width, wide_two = tokens.shape[1], two_own.shape[1]
    heads, heads_two = fine_bias.shape[0], coarse_bias.shape[0]
    size = width // heads
    scale = size ** (-0.5) * LOG2E
    around = Around()
    lons, lvls = lax.axis_size("lon"), lax.axis_size("lvl")
    gather = Gather((s0, s1, s2, s3, s4), (f0, f1, f2, f3, f4), units, split, sems)
    block_of = gather.block_of
    halo = Halo(around, fine, own, wide, send1, recv1)
    halo_two = Halo(around, coarse, two_own, two_wide, send2, recv2)
    barrier = pltpu.get_barrier_semaphore()
    peers = around.greet(barrier) + gather.greet(barrier)
    brought = (
        fine_tags, coarse_tags, lane_ref, fine_gain, index_ref, fine_table, coarse_table, number_ref, merge_gain,
        coarse_gain,
    )
    fetches = [pltpu.make_async_copy(src, dst, local.at[2 + n]) for n, (src, dst) in enumerate(zip(small, brought))]
    for fetch in fetches[:3]:
        fetch.start()
    fetch = pltpu.make_async_copy(tokens_ref, tokens, local.at[0])
    fetch.start()
    for other in fetches[3:]:
        other.start()
    halo.clear()
    halo_two.clear()
    for side, (dy, dx) in enumerate(AROUND):
        if dy:
            def clear(side=side):
                tag_wide[side] = jnp.zeros(tag_wide.shape[1:], tag_wide.dtype)
            pl.when(jnp.logical_not(around.there(dy)))(clear)
    pl.semaphore_wait(barrier, peers)
    gather.begin()
    for other in fetches[:3]:
        other.wait()
    fine_lanes = fine.across * LANES
    coarse_lanes = coarse.across * LANES
    top = tag_rows(fine, fine_tags, lane_ref[0:1, :fine_lanes], lane_ref[1:2, :fine_lanes], fine_lanes)
    spare = jnp.zeros((tag_own.shape[0] - fine.quads - coarse.quads, LANES), jnp.float32)
    low = tag_rows(coarse, coarse_tags, lane_ref[0:1, fine_lanes:], lane_ref[1:2, fine_lanes:], coarse_lanes)
    tag_own[...] = jnp.concatenate([top, low, spare], axis=0).astype(jnp.bfloat16)

    def tag_copy(side):
        dy, dx = AROUND[side]
        return around.copy(tag_own, tag_wide.at[side], tag_send.at[side], tag_recv.at[side], dy, dx)

    for side, (dy, dx) in enumerate(AROUND):
        around.when_there(-dy, lambda side=side: tag_copy(side).start())

    fetch.wait()
    fetches[3].wait()
    fetches[4].wait()
    normed = normalize(tokens[...], fine_gain[...])
    arranged = pick(index_ref[: fine.quads * ROWS, 0:1], normed)
    own[...] = arranged
    halo.start()
    for q in range(fine.quads):
        spot = fine.spot(*divmod(q, fine.across))
        wide[pl.ds(spot * ROWS, ROWS), :] = arranged[q * ROWS : (q + 1) * ROWS]

    for other in fetches[5:]:
        other.wait()
    parts = split_table((fine_table, coarse_table), padded)
    fine_bias[...] = jnp.zeros_like(fine_bias)
    coarse_bias[...] = jnp.zeros_like(coarse_bias)
    chunk = 4 * QUAD // 6
    for first in range(0, 4 * QUAD, chunk):
        fill_bias(parts, number_ref, (fine_bias, coarse_bias), first, first + chunk)
        if first:
            gather.step()

    for side, (dy, dx) in enumerate(AROUND):
        around.when_there(dy, lambda side=side: tag_copy(side).wait_recv())
    tags = [tag_wide[side].astype(jnp.float32) for side in range(len(AROUND))] + [tag_own[...].astype(jnp.float32)]
    fill_masks(fine, tags, 0, fine_masks)
    fill_masks(coarse, tags, fine.quads, coarse_masks)

    gather.ready(0)
    half = width // lvls
    for lvl in range(lvls):
        part = jnp.dot(turned(own, slice(None), block_of, lons), flat(f0[lvl, 0]), preferred_element_type=jnp.float32)
        query[:, lvl * half : (lvl + 1) * half] = (part * scale).astype(jnp.bfloat16)
    halo.finish()
    for member, target in ((1, keys), (2, values)):
        gather.ready(member)

        @pl.loop(0, fine.windows // fine.columns)
        def _(band):
            count = fine.columns * WINDOW
            rows = pl.ds(pl.multiple_of(band * count, count), count)
            x = turned(wide, rows, block_of, lons)
            for lvl in range(lvls):
                part = jnp.dot(x, flat(f0[lvl, member]), preferred_element_type=jnp.float32)
                target[rows, lvl * half : (lvl + 1) * half] = part.astype(jnp.bfloat16)

    per_row = fine.across
    for first in range(0, fine.quads, per_row):
        @pl.loop(first, first + per_row, step=2)
        def _(q):
            attend(
                fine, [(q + i, group) for i in range(2) for group in range(width // LANES)], query, keys, values,
                fine_bias, fine_masks, mixed, size,
            )
        gather.step()

    own_mixed = pick(index_ref[: fine.own, 1:2], mixed[...])
    gather.ready(3)
    update = None
    for lvl in range(lvls):
        term = lax.dot_general(
            own_mixed[:, lvl * half : (lvl + 1) * half], flat(f1[lvl, 0]), NT, preferred_element_type=jnp.float32
        )
        update = term if update is None else update + term

    def put_fine(cols, value):
        fine_value[:, cols] = (tokens[:, cols].astype(jnp.float32) + value).astype(jnp.bfloat16)

    turn_back(update, block_of, lons, put_fine)
    publish = pltpu.make_async_copy(fine_value, fine_ref, local.at[1])
    publish.start()

    count = coarse.quads * ROWS
    stacked = pick(index_ref[: 4 * count, 2:3], fine_value[...]).astype(jnp.float32)
    members = [stacked[m * count : (m + 1) * count] for m in range(4)]
    mean = sum(jnp.sum(m, axis=-1, keepdims=True) for m in members) / (4 * width)
    centers = [m - mean for m in members]
    spread = sum(jnp.sum(c * c, axis=-1, keepdims=True) for c in centers) / (4 * width)
    factor = lax.rsqrt(spread + EPSILON)
    normed = jnp.concatenate(
        [(centers[m] * factor * merge_gain[:, m * width : (m + 1) * width]).astype(jnp.bfloat16) for m in range(4)],
        axis=1,
    )
    merged = None
    share = 4 * width // lvls
    for u in [u for u in range(len(units)) if units[u][0] == 2]:
        gather.ready(u)
        _, _, _, col, cols = units[u]
        for lvl in range(lvls):
            start = lvl * share + col
            term = lax.dot_general(
                normed[:, start : start + cols], flat(f2[lvl, 0, :, :, col : col + cols]), NT,
                preferred_element_type=jnp.float32,
            )
            merged = term if merged is None else merged + term

    def put_coarse(cols, value):
        two_in[:, cols] = value.astype(jnp.bfloat16)

    turn_back(merged, block_of, lons, put_coarse)
    two_own[...] = normalize(two_in[...], coarse_gain[...])
    halo_two.start()
    for q in range(coarse.quads):
        spot = coarse.spot(*divmod(q, coarse.across))
        two_wide[pl.ds(spot * ROWS, ROWS), :] = two_own[q * ROWS : (q + 1) * ROWS, :]
    gather.step(2)
    halo_two.finish()

    share = wide_two // lvls
    inner = [u for u in range(len(units)) if units[u][0] == 3]
    for u in inner:
        gather.ready(u)
        _, _, _, col, cols = units[u]
        for lvl in range(lvls):
            start = lvl * share + col
            part = jnp.dot(
                turned(two_own, slice(None), block_of, lons), flat(f3[lvl, 0, :, :, col : col + cols]),
                preferred_element_type=jnp.float32,
            )
            two_query[:, start : start + cols] = (part * scale).astype(jnp.bfloat16)
            weight = jnp.concatenate([flat(f3[lvl, k, :, :, col : col + cols]) for k in (1, 2)], axis=1)
            part = jnp.dot(
                turned(two_wide, slice(None), block_of, lons), weight, preferred_element_type=jnp.float32
            ).astype(jnp.bfloat16)
            two_keys[:, start : start + cols] = part[:, :cols]
            two_values[:, start : start + cols] = part[:, cols:]

        attend(
            coarse, [(q, (lvl * share + col) // LANES) for q in range(coarse.quads) for lvl in range(lvls)],
            two_query, two_keys, two_values, coarse_bias, coarse_masks, two_mixed, size,
        )

    update = None
    for u in [u for u in range(len(units)) if units[u][0] == 4]:
        gather.ready(u)
        _, _, _, col, cols = units[u]
        for lvl in range(lvls):
            start = lvl * share + col
            term = lax.dot_general(
                two_mixed[:, start : start + cols], flat(f4[lvl, 0, :, :, col : col + cols]), NT,
                preferred_element_type=jnp.float32,
            )
            update = term if update is None else update + term

    def put_out(cols, value):
        two_value[:, cols] = (two_in[:, cols].astype(jnp.float32) + value).astype(jnp.bfloat16)

    turn_back(update, block_of, lons, put_out)
    pitch = up_to(coarse.lon_len, 16)
    result = pick(index_ref[: coarse.lat_len * pitch, 3:4], two_value[...])
    for r in range(coarse.lat_len):
        coarse_ref[r] = result[r * pitch : r * pitch + coarse.lon_len]

    publish.wait()
    gather.end()
    for side, (dy, dx) in enumerate(AROUND):
        around.when_there(-dy, lambda side=side: tag_copy(side).wait_send())
    halo.drain()
    halo_two.drain()


def publish_kernel(fine_in, coarse_in, fine_out, coarse_out, fine_held, coarse_held, sems):
    steps = ((fine_in, fine_held, fine_out), (coarse_in, coarse_held, coarse_out))
    come = [pltpu.make_async_copy(a, b, sems.at[n]) for n, (a, b, _) in enumerate(steps)]
    leave = [pltpu.make_async_copy(b, c, sems.at[2 + n]) for n, (_, b, c) in enumerate(steps)]
    for copy in come:
        copy.start()
    for n in range(2):
        come[n].wait()
        leave[n].start()
    for copy in leave:
        copy.wait()


def level_scratch(plan, features, heads):
    rows, all_rows = plan.quads * ROWS, plan.windows * WINDOW
    return [
        pltpu.VMEM((rows, features), jnp.bfloat16),
        pltpu.VMEM((all_rows, features), jnp.bfloat16),
        pltpu.VMEM((rows, features), jnp.bfloat16),
        pltpu.VMEM((all_rows, features), jnp.bfloat16),
        pltpu.VMEM((all_rows, features), jnp.bfloat16),
        pltpu.VMEM((rows, features), jnp.bfloat16),
        pltpu.VMEM((heads, WINDOW, LANES), jnp.float32),
        pltpu.VMEM((plan.quads, ROWS, LANES), jnp.float32),
    ]


def shards(
    tokens, fine_tags, coarse_tags, fine_gain, fine_inward, fine_outward, fine_table, merge_gain,
    merge_weight, coarse_gain, coarse_inward, coarse_outward, coarse_table,
):
    _, lat_len, lon_len, width = tokens.shape
    fine, coarse = Plan(lat_len, lon_len), Plan(lat_len // 2, lon_len // 2)
    weights = [fine_inward, fine_outward[None], merge_weight[None], coarse_inward, coarse_outward[None]]
    grps, lats, lons, lvls = (lax.axis_size(a) for a in ("grp", "lat", "lon", "lvl"))
    split = grps == 2 and lats == 2 and all(w.shape[1] % LANES == 0 for w in weights)
    units = weight_units(weights)
    wide_two = coarse_inward.shape[1] * lons
    heads, heads_two = fine_table.shape[0], coarse_table.shape[0]
    pitch = up_to(coarse.lon_len, 16)

    columns = [fine.natural(), fine.back(fine.lon_len), patches(fine, coarse), coarse.back(pitch)]
    index = np.full((max(len(c) for c in columns), len(columns)), -1, np.int32)
    for n, column in enumerate(columns):
        index[: len(column), n] = column
    lane = np.concatenate([np.stack(p.lanes()) for p in (fine, coarse)], axis=1).astype(np.int32)

    small = [
        fine_tags.reshape(lat_len, 1, lon_len), coarse_tags.reshape(coarse.lat_len, 1, coarse.lon_len), lane,
        fine_gain[None], index, fine_table, coarse_table, offset_numbers(), merge_gain[None], coarse_gain[None],
    ]
    dma = pltpu.SemaphoreType.DMA
    bf16 = jnp.bfloat16
    sides, tag_count = len(AROUND), up_to(fine.quads + coarse.quads, 16)
    fine_out, coarse_out = pl.pallas_call(
        functools.partial(kernel, fine, coarse, units, split),
        out_shape=[
            jax.ShapeDtypeStruct((fine.own, width), bf16),
            jax.ShapeDtypeStruct((coarse.lat_len, coarse.lon_len, wide_two), bf16),
        ],
        in_specs=[HBM] * (1 + SMALL + len(weights)),
        out_specs=[ANY, VMEM],
        scratch_shapes=[pltpu.VMEM(x.shape, x.dtype) for x in small]
        + [pltpu.VMEM((fine.own, width), bf16)]
        + level_scratch(fine, width, heads)
        + [pltpu.VMEM((fine.own, width), bf16)]
        + level_scratch(coarse, wide_two, heads_two)
        + [pltpu.VMEM((coarse.quads * ROWS, wide_two), bf16)] * 2
        + [
            pltpu.VMEM((heads + heads_two, up_to(fine_table.shape[1], LANES)), jnp.float32),
            pltpu.VMEM((tag_count, LANES), bf16),
            pltpu.VMEM((sides, tag_count, LANES), bf16),
        ]
        + [pltpu.VMEM((lvls, w.shape[0], lons, w.shape[1], w.shape[2]), bf16) for w in weights]
        + [dma((2 + SMALL,)), dma((sides,)), dma((sides,))]
        + [dma((len(fine.halo),))] * 2
        + [dma((len(coarse.halo),))] * 2
        + gather_scratch(units),
        compiler_params=pltpu.CompilerParams(collective_id=1, has_side_effects=True, vmem_limit_bytes=LIMIT),
        name="levels",
    )(
        tokens.reshape(fine.own, width), *small, *weights,
    )
    fine_out, coarse_out = pl.pallas_call(
        publish_kernel,
        out_shape=[jax.ShapeDtypeStruct(x.shape, x.dtype) for x in (fine_out, coarse_out)],
        in_specs=[HBM] * 2,
        out_specs=[HBM] * 2,
        scratch_shapes=[pltpu.VMEM(x.shape, x.dtype) for x in (fine_out, coarse_out)] + [dma((4,))],
        name="publish",
    )(fine_out, coarse_out)
    return fine_out.reshape(tokens.shape), coarse_out[None]


def solution(mesh):
    placed = (
        P(("grp", "lvl"), "lat", "lon", None),
        P(("grp", "lvl"), "lat", "lon"),
        P(("grp", "lvl"), "lat", "lon"),
        P(),
        P(None, "lon", "lvl"),
        P("lon", "lvl"),
        P(),
        P(),
        P("lon", "lvl"),
        P(),
        P(None, "lon", "lvl"),
        P("lon", "lvl"),
        P(),
    )
    return jax.shard_map(
        shards,
        mesh=mesh,
        in_specs=placed,
        out_specs=(P(("grp", "lvl"), "lat", "lon", None), P(("grp", "lvl"), "lat", "lon", None)),
        check_vma=False,
    )
```

```python
import functools
import math

import jax
import jax.numpy as jnp
import numpy as np
from jax import lax
from jax.experimental import pallas as pl
from jax.experimental.pallas import tpu as pltpu
from jax.sharding import PartitionSpec as P

WIN_LAT = 6
WIN_LON = 12
HALF_LAT = WIN_LAT // 2
HALF_LON = WIN_LON // 2
QUAD = HALF_LAT * HALF_LON
ROWS = -(-QUAD // 16) * 16
SENT = -(-QUAD // 8) * 8
WINDOW = 4 * ROWS
EPSILON = 1e-05
LANES = 128
LOG2E = math.log2(math.e)
MESH = pl.DeviceIdType.MESH
VMEM = pl.BlockSpec(memory_space=pltpu.VMEM)
ANY = pl.BlockSpec(memory_space=pl.ANY)
HBM = pl.BlockSpec(memory_space=pltpu.HBM)
LIMIT = 60 * 1024 * 1024
NT = (((1,), (1,)), ((), ()))
AROUND = ((0, -1), (0, 1), (-1, 0), (1, 0), (-1, -1), (-1, 1), (1, -1), (1, 1))
AHEAD = 3
LAG = 2
RELAYED = 3
ORDER = (1, 3, 2)
MERGE = 256
LAST = 256
SMALL = 10
FIRST = (32, 48)


def up_to(count, step):
    return -(-count // step) * step


class Plan:
    def __init__(self, lat_len, lon_len):
        self.lat_len, self.lon_len = lat_len, lon_len
        self.own = lat_len * lon_len
        self.down, self.across = lat_len // HALF_LAT, lon_len // HALF_LON
        self.quads = self.down * self.across
        self.columns = self.across // 2 + 1
        self.windows = (self.down // 2 + 1) * self.columns
        self.halo = []
        for side, (dy, dx) in enumerate(AROUND):
            rows = [-1] if dy < 0 else ([self.down] if dy > 0 else range(self.down))
            cols = [-1] if dx < 0 else ([self.across] if dx > 0 else range(self.across))
            for r in rows:
                for c in cols:
                    self.halo.append((side, r, c, (r % self.down) * self.across + c % self.across))

    def spot(self, r, c):
        window = ((r + 1) // 2) * self.columns + (c + 1) // 2
        return 4 * window + ((r + 1) % 2) * 2 + (c + 1) % 2

    def natural(self):
        result = np.full((self.quads * ROWS,), -1, np.int32)
        for q in range(self.quads):
            for p in range(QUAD):
                r = (q // self.across) * HALF_LAT + p // HALF_LON
                c = (q % self.across) * HALF_LON + p % HALF_LON
                result[q * ROWS + p] = r * self.lon_len + c
        return result

    def back(self, pitch):
        result = np.full((self.lat_len * pitch,), -1, np.int32)
        for row, token in enumerate(self.natural()):
            if token >= 0:
                result[token // self.lon_len * pitch + token % self.lon_len] = row
        return result

    def lanes(self):
        lane = np.arange(self.across * LANES)
        place = lane % ROWS
        column = (lane // LANES) * HALF_LON + place % HALF_LON
        return np.where(place < QUAD, column, -1), np.where(place < QUAD, place // HALF_LON, -1)


def patches(fine, coarse):
    token = coarse.natural()
    result = []
    for s in range(2):
        for t in range(2):
            a, b = token // coarse.lon_len, token % coarse.lon_len
            result.append(np.where(token >= 0, (2 * a + s) * fine.lon_len + 2 * b + t, -1))
    return np.concatenate(result)


def offset_numbers():
    spot = np.arange(WINDOW)
    place = spot % ROWS
    r = spot // ROWS // 2 * HALF_LAT + place // HALF_LON
    c = spot // ROWS % 2 * HALF_LON + place % HALF_LON
    number = (r[:, None] - r[None, :] + WIN_LAT - 1) * (2 * WIN_LON - 1) + c[:, None] - c[None, :] + WIN_LON - 1
    valid = (place < QUAD)[:, None] & (place < QUAD)[None, :]
    return np.where(valid, number, -1).astype(np.int32)


def onehot(index, width):
    spots = lax.broadcasted_iota(jnp.int32, (index.shape[0], width), 1)
    return jnp.where(spots == index, 1.0, 0.0).astype(jnp.bfloat16)


def pick(index, source):
    return jnp.dot(
        onehot(index, source.shape[0]), source, preferred_element_type=jnp.float32
    ).astype(jnp.bfloat16)


def normalize(values, gain):
    widened = values.astype(jnp.float32)
    center = widened - jnp.mean(widened, axis=-1, keepdims=True)
    spread = jnp.mean(center * center, axis=-1, keepdims=True)
    return (center * lax.rsqrt(spread + EPSILON) * gain).astype(jnp.bfloat16)


class Around:
    def __init__(self):
        self.lat, self.lon = lax.axis_index("lat"), lax.axis_index("lon")
        self.lats, self.lons = lax.axis_size("lat"), lax.axis_size("lon")

    def place(self, dy, dx):
        return {
            "lat": lax.rem(self.lat + dy + self.lats, self.lats),
            "lon": lax.rem(self.lon + dx + self.lons, self.lons),
        }

    def there(self, dy):
        return (self.lat > 0) if dy < 0 else (self.lat < self.lats - 1)

    def when_there(self, dy, action):
        if dy == 0:
            action()
        else:
            pl.when(self.there(dy))(action)

    def greet(self, barrier):
        for dy, dx in AROUND:
            def signal(dy=dy, dx=dx):
                pl.semaphore_signal(barrier, inc=1, device_id=self.place(dy, dx), device_id_type=MESH)
            self.when_there(dy, signal)
        return 2 + 3 * (self.lat > 0).astype(jnp.int32) + 3 * (self.lat < self.lats - 1).astype(jnp.int32)

    def copy(self, src, dst, send, recv, dy, dx):
        return pltpu.make_async_remote_copy(
            src_ref=src, dst_ref=dst, send_sem=send, recv_sem=recv,
            device_id=self.place(-dy, -dx), device_id_type=MESH,
        )


class Halo:
    def __init__(self, around, plan, own, wide, send, recv):
        self.around, self.plan, self.own, self.wide, self.send, self.recv = around, plan, own, wide, send, recv

    def copy(self, n):
        side, r, c, q = self.plan.halo[n]
        return self.around.copy(
            self.own.at[pl.ds(q * ROWS, SENT)], self.wide.at[pl.ds(self.plan.spot(r, c) * ROWS, SENT)],
            self.send.at[n], self.recv.at[n], *AROUND[side],
        )

    def clear(self):
        for side, r, c, _ in self.plan.halo:
            start, dy = self.plan.spot(r, c) * ROWS, AROUND[side][0]
            if SENT < ROWS:
                spare = pl.ds(start + SENT, ROWS - SENT)
                self.wide[spare, :] = jnp.zeros((ROWS - SENT, self.wide.shape[1]), self.wide.dtype)
            if dy:
                def beyond(start=start):
                    self.wide[pl.ds(start, SENT), :] = jnp.zeros((SENT, self.wide.shape[1]), self.wide.dtype)
                pl.when(jnp.logical_not(self.around.there(dy)))(beyond)

    def start(self):
        for n, (side, *_) in sorted(enumerate(self.plan.halo), key=lambda item: -abs(AROUND[item[1][0]][0])):
            self.around.when_there(-AROUND[side][0], lambda n=n: self.copy(n).start())

    def finish(self):
        for n, (side, *_) in enumerate(self.plan.halo):
            self.around.when_there(AROUND[side][0], lambda n=n: self.copy(n).wait_recv())

    def drain(self):
        for n, (side, *_) in enumerate(self.plan.halo):
            self.around.when_there(-AROUND[side][0], lambda n=n: self.copy(n).wait_send())


class Gather:
    def __init__(self, shards, fulls, units, split, sems):
        self.shards, self.fulls, self.units, self.split, self.sems = shards, fulls, units, split, sems
        self.index = {a: lax.axis_index(a) for a in ("grp", "lat", "lon", "lvl")}
        self.size = {a: lax.axis_size(a) for a in ("grp", "lat", "lon", "lvl")}
        self.slots = range(1, self.size["lon"])
        self.plane = ("lat", "grp")
        self.line = split and self.size["lon"] == 4
        self.now = self.arrived = self.forwarded = self.shared = 0

    def at(self, axis, step):
        return {axis: lax.rem(self.index[axis] + step + self.size[axis], self.size[axis])}

    def greet(self, barrier):
        peers = 0
        for axis in ("lon", "lvl", "lat", "grp") if self.split else ("lon", "lvl"):
            for d in range(1, self.size[axis]):
                pl.semaphore_signal(barrier, inc=1, device_id=self.at(axis, d), device_id_type=MESH)
                peers += 1
        return peers

    def block_of(self, slot):
        return lax.rem(self.index["lon"] + slot, self.size["lon"]) if self.split else slot

    def rows(self, u):
        return self.shards[self.units[u][0]].shape[1]

    def piece(self, u, other=None):
        if not self.split:
            return 0, self.rows(u)
        size = self.rows(u) // 4
        lat, grp = [1 - self.index[a] if a == other else self.index[a] for a in self.plane]
        return pl.multiple_of((lat * 2 + grp) * size, 16), size

    def held(self, u, start, size):
        m, k, depth, col, cols = self.units[u]
        return self.shards[m].at[pl.ds(k, depth), pl.ds(start, size), pl.ds(col, cols)]

    def block(self, u, slot, slots, start, size):
        m, k, depth, col, cols = self.units[u]
        return self.fulls[m].at[
            self.index["lvl"], pl.ds(k, depth), pl.ds(slot, slots), pl.ds(start, size), pl.ds(col, cols)
        ]

    def slot(self, u, slot, start, size):
        m, k, depth, col, cols = self.units[u]
        return self.fulls[m].at[self.index["lvl"], pl.ds(k, depth), slot, pl.ds(start, size), pl.ds(col, cols)]

    def remote(self, src, dst, kind, number, device):
        send, recv = self.sems[1 + 2 * kind], self.sems[2 + 2 * kind]
        return pltpu.make_async_remote_copy(
            src_ref=src, dst_ref=dst, send_sem=send.at[number], recv_sem=recv.at[number],
            device_id=device, device_id_type=MESH,
        )

    def own_copy(self, u):
        slot = 0 if self.split else self.index["lon"]
        return pltpu.make_async_copy(
            self.held(u, 0, self.rows(u)), self.slot(u, slot, 0, self.rows(u)), self.sems[0].at[u]
        )

    def lon_copy(self, u, s):
        start, size = self.piece(u)
        slot = s if self.split else self.index["lon"]
        return self.remote(
            self.held(u, start, size), self.slot(u, slot, start, size), 0, (u, s - 1), self.at("lon", -s)
        )

    def near_copy(self, u, n):
        block = self.block(u, 1, self.size["lon"] - 1, *self.piece(u))
        return self.remote(block, block, 1, (u, n), self.at(self.plane[n], 1))

    def far_copy(self, u, n):
        start, size = self.piece(u, self.plane[n])
        cut = size * FIRST[u % len(FIRST)] // 64 // 16 * 16
        start, size = (start, cut) if n == 0 else (pl.multiple_of(start + cut, 16), size - cut)
        block = self.block(u, 1, self.size["lon"] - 1, start, size)
        return self.remote(block, block, 2, (u, n), self.at(self.plane[1 - n], 1))

    def lvl_copy(self, u):
        block = self.block(u, 0, self.size["lon"], 0, self.rows(u))
        return self.remote(block, block, 3, (u,), self.at("lvl", 1))

    def relayed(self, u):
        return self.line and RELAYED <= u < len(self.units)

    def direct(self, u, s, action):
        if s == 2 or not self.relayed(u):
            action()
        else:
            pl.when(self.index["lon"] > 0 if s == 1 else self.index["lon"] < 3)(action)

    def relays(self, u, action):
        for lon, slot, step in ((2, 1, 1), (1, 3, -1)) if self.relayed(u) else ():
            def act(slot=slot, step=step):
                place = self.piece(u)
                action(pltpu.make_async_remote_copy(
                    src_ref=self.slot(u, 2, *place), dst_ref=self.slot(u, slot, *place),
                    send_sem=self.sems[9].at[u], recv_sem=self.sems[2].at[u, slot - 1],
                    device_id=self.at("lon", step), device_id_type=MESH,
                ))
            pl.when(self.index["lon"] == lon)(act)

    def relay(self, u):
        if self.relayed(u):
            self.lon_copy(u, 2).wait_recv()
            self.relays(u, lambda copy: copy.start())

    def issue(self, u):
        if u < len(self.units):
            for s in ORDER if self.line else self.slots:
                self.direct(u, s, lambda s=s: self.lon_copy(u, s).start())
            self.own_copy(u).start()

    def begin(self):
        for u in range(AHEAD):
            self.issue(u)

    def arrive(self):
        u = self.arrived
        self.arrived += 1
        for s in self.slots:
            if s != 2 or not self.relayed(u):
                self.lon_copy(u, s).wait_recv()
        if self.split:
            for n in range(2):
                self.near_copy(u, n).start()
        self.issue(u + AHEAD)

    def forward(self):
        u = self.forwarded
        self.forwarded += 1
        if self.split:
            for n in range(2):
                self.near_copy(u, n).wait_recv()
                self.far_copy(u, n).start()

    def share(self):
        u = self.shared
        self.shared += 1
        if self.split:
            for n in range(2):
                self.far_copy(u, n).wait_recv()
        self.own_copy(u).wait()
        self.lvl_copy(u).start()

    def step(self, times=1):
        for _ in range(times):
            k, count = self.now, len(self.units)
            self.now += 1
            if 0 <= k - LAG < count:
                self.forward()
            if 0 <= k - 2 * LAG < count:
                self.share()
            if k < count:
                self.arrive()
            self.relay(k + 1)

    def ready(self, u):
        while self.shared <= u:
            self.step()
        self.lvl_copy(u).wait_recv()

    def end(self):
        for u in range(len(self.units)):
            self.lvl_copy(u).wait_send()
            for s in self.slots:
                self.direct(u, s, lambda s=s: self.lon_copy(u, s).wait_send())
            self.relays(u, lambda copy: copy.wait_send())
            if self.split:
                for n in range(2):
                    self.near_copy(u, n).wait_send()
                    self.far_copy(u, n).wait_send()


def weight_units(shards):
    fine_inward, fine_outward, merge, coarse_inward, coarse_outward = [s.shape for s in shards]
    units = [(0, k, 1, 0, fine_inward[2]) for k in range(3)]
    units.append((1, 0, 1, 0, fine_outward[2]))
    units += [(2, 0, 1, c, MERGE) for c in range(0, merge[2], MERGE)]
    units += [(3, 0, 3, c, LANES) for c in range(0, coarse_inward[2], LANES)]
    units += [(4, 0, 1, c, LAST) for c in range(0, coarse_outward[2], LAST)]
    return units


def gather_scratch(units):
    count, lons = len(units), lax.axis_size("lon")
    dma = pltpu.SemaphoreType.DMA
    return [dma((count,))] + [dma((count, lons - 1))] * 2 + [dma((count, 2))] * 4 + [dma((count,))] * 3


def flat(block):
    return block.reshape(block.shape[0] * block.shape[1], block.shape[2])


def turned(ref, rows, block_of, slots):
    size = ref.shape[1] // slots
    if size % LANES:
        return ref[rows, :]
    return jnp.concatenate(
        [ref[rows, pl.ds(pl.multiple_of(block_of(s) * size, size), size)] for s in range(slots)], axis=1
    )


def turn_back(value, block_of, slots, store):
    size = value.shape[1] // slots
    if size % LANES:
        store(slice(None), value)
        return
    for s in range(slots):
        store(pl.ds(pl.multiple_of(block_of(s) * size, size), size), value[:, s * size : (s + 1) * size])


def tag_rows(plan, tags_ref, column, place, features):
    grid = jnp.concatenate([tags_ref[r].astype(jnp.float32) for r in range(plan.lat_len)], axis=0)
    spots = lax.broadcasted_iota(jnp.int32, (plan.lon_len, features), 0)
    hot = jnp.where(spots == column, 1.0, 0.0).astype(jnp.bfloat16)
    spread = jnp.dot(grid.astype(jnp.bfloat16), hot, preferred_element_type=jnp.float32)
    rows = []
    for q in range(plan.down):
        row = jnp.zeros((1, features), jnp.float32)
        for k in range(HALF_LAT):
            r = q * HALF_LAT + k
            row = jnp.where(place == k, spread[r : r + 1, :], row)
        rows.append(row)
    return jnp.concatenate(
        [row[:, c * LANES : (c + 1) * LANES] for row in rows for c in range(plan.across)], axis=0
    )


def fill_masks(plan, tags, offset, masks):
    lane = lax.broadcasted_iota(jnp.int32, (ROWS, LANES), 1)
    row = lax.broadcasted_iota(jnp.int32, (ROWS, LANES), 0)
    owner = lax.broadcasted_iota(jnp.int32, (1, LANES), 1) // ROWS

    def tag_row(r, c):
        dy = -1 if r < 0 else int(r >= plan.down)
        dx = -1 if c < 0 else int(c >= plan.across)
        side = AROUND.index((dy, dx)) if dy or dx else len(AROUND)
        row = offset + r % plan.down * plan.across + c % plan.across
        return tags[side][row : row + 1]

    for q in range(plan.quads):
        r, c = divmod(q, plan.across)
        top, left = r - (r + 1) % 2, c - (c + 1) % 2
        across = tag_row(top, left)
        for a in range(1, 4):
            across = jnp.where(owner == a, tag_row(top + a // 2, left + a % 2), across)
        down = jnp.sum(jnp.where(lane == row, tag_row(r, c), 0.0), axis=-1, keepdims=True)
        masks[q] = jnp.where(down == across, 0.0, -1e30)


def split_table(tables, padded):
    padded[...] = jnp.zeros_like(padded)
    start = 0
    for table in tables:
        heads, entries = table.shape
        padded[start : start + heads, :entries] = table[...] * LOG2E
        start += heads
    rest, terms = padded[...], []
    for _ in range(3):
        term = rest.astype(jnp.bfloat16)
        terms.append(term)
        rest = rest - term.astype(jnp.float32)
    return jnp.concatenate(terms, axis=0)


def fill_bias(parts, number_ref, biases, first, last):
    total = parts.shape[0] // 3
    spots = lax.broadcasted_iota(jnp.int32, (parts.shape[1], LANES), 0)
    for p in range(first, last):
        row = p // QUAD * ROWS + p % QUAD
        hot = jnp.where(spots == number_ref[row : row + 1, :], 1.0, 0.0).astype(jnp.bfloat16)
        terms = jnp.dot(parts, hot, preferred_element_type=jnp.float32)
        value = terms[:total] + terms[total : 2 * total] + terms[2 * total :]
        start = 0
        for bias in biases:
            bias[:, row, :] = value[start : start + bias.shape[0]]
            start += bias.shape[0]


def attend(plan, spots, query, keys, values, bias_ref, masks, mixed, size):
    heads = LANES // size
    owner = lax.broadcasted_iota(jnp.int32, (ROWS, LANES), 1) // size
    ones = jnp.ones((WINDOW, LANES), jnp.bfloat16)
    where, scores, weights, both = [], [], [], []
    for q, group in spots:
        r = lax.div(q, plan.across)
        c = q - r * plan.across
        window = lax.div(r + 1, 2) * plan.columns + lax.div(c + 1, 2)
        place = lax.rem(r + 1, 2) * 2 + lax.rem(c + 1, 2)
        where.append((
            q, group, pl.ds(pl.multiple_of(q * ROWS, ROWS), ROWS), pl.ds(pl.multiple_of(window * WINDOW, WINDOW), WINDOW),
            pl.ds(pl.multiple_of(place * ROWS, ROWS), ROWS), slice(group * LANES, (group + 1) * LANES),
        ))
    for q, group, rows, others, inside, cols in where:
        block = query[rows, cols]
        stack = jnp.concatenate([jnp.where(owner == h, block, jnp.zeros_like(block)) for h in range(heads)], axis=0)
        scores.append(lax.dot_general(stack, keys[others, cols], NT, preferred_element_type=jnp.float32))
    for (q, group, rows, others, inside, cols), score in zip(where, scores):
        bias = bias_ref[group * heads : (group + 1) * heads, inside, :].reshape(heads * ROWS, LANES)
        score = score + bias + jnp.concatenate([masks[q]] * heads, axis=0)
        weights.append(jnp.exp2(score - jnp.max(score, axis=-1, keepdims=True)).astype(jnp.bfloat16))
    for (q, group, rows, others, inside, cols), weight in zip(where, weights):
        both.append(jnp.dot(
            weight, jnp.concatenate([values[others, cols], ones], axis=1), preferred_element_type=jnp.float32
        ))
    for (q, group, rows, others, inside, cols), part in zip(where, both):
        blended, totals = part[:ROWS, :LANES], part[:ROWS, LANES:]
        for h in range(1, heads):
            result = part[h * ROWS : (h + 1) * ROWS]
            blended = jnp.where(owner == h, result[:, :LANES], blended)
            totals = jnp.where(owner == h, result[:, LANES:], totals)
        mixed[rows, cols] = (blended / totals).astype(jnp.bfloat16)


def kernel(
    fine, coarse, units, split, tokens_ref, *refs,
):
    run(fine, coarse, units, split, tokens_ref, refs[:SMALL], *refs[SMALL:])


def run(
    fine, coarse, units, split, tokens_ref, small, s0, s1, s2, s3, s4, fine_ref, coarse_ref,
    fine_tags, coarse_tags, lane_ref, fine_gain, index_ref, fine_table, coarse_table, number_ref, merge_gain,
    coarse_gain, tokens, own, wide, query, keys, values, mixed, fine_bias, fine_masks, fine_value,
    two_own, two_wide, two_query, two_keys, two_values, two_mixed, coarse_bias, coarse_masks, two_in, two_value,
    padded, tag_own, tag_wide, f0, f1, f2, f3, f4, local, tag_send, tag_recv, send1, recv1, send2, recv2, *sems,
):
    width, wide_two = tokens.shape[1], two_own.shape[1]
    heads, heads_two = fine_bias.shape[0], coarse_bias.shape[0]
    size = width // heads
    scale = size ** (-0.5) * LOG2E
    around = Around()
    lons, lvls = lax.axis_size("lon"), lax.axis_size("lvl")
    gather = Gather((s0, s1, s2, s3, s4), (f0, f1, f2, f3, f4), units, split, sems)
    block_of = gather.block_of
    halo = Halo(around, fine, own, wide, send1, recv1)
    halo_two = Halo(around, coarse, two_own, two_wide, send2, recv2)
    barrier = pltpu.get_barrier_semaphore()
    peers = around.greet(barrier) + gather.greet(barrier)
    brought = (
        fine_tags, coarse_tags, lane_ref, fine_gain, index_ref, fine_table, coarse_table, number_ref, merge_gain,
        coarse_gain,
    )
    fetches = [pltpu.make_async_copy(src, dst, local.at[2 + n]) for n, (src, dst) in enumerate(zip(small, brought))]
    for fetch in fetches[:3]:
        fetch.start()
    fetch = pltpu.make_async_copy(tokens_ref, tokens, local.at[0])
    fetch.start()
    for other in fetches[3:]:
        other.start()
    halo.clear()
    halo_two.clear()
    for side, (dy, dx) in enumerate(AROUND):
        if dy:
            def clear(side=side):
                tag_wide[side] = jnp.zeros(tag_wide.shape[1:], tag_wide.dtype)
            pl.when(jnp.logical_not(around.there(dy)))(clear)
    pl.semaphore_wait(barrier, peers)
    gather.begin()
    for other in fetches[:3]:
        other.wait()
    fine_lanes = fine.across * LANES
    coarse_lanes = coarse.across * LANES
    top = tag_rows(fine, fine_tags, lane_ref[0:1, :fine_lanes], lane_ref[1:2, :fine_lanes], fine_lanes)
    spare = jnp.zeros((tag_own.shape[0] - fine.quads - coarse.quads, LANES), jnp.float32)
    low = tag_rows(coarse, coarse_tags, lane_ref[0:1, fine_lanes:], lane_ref[1:2, fine_lanes:], coarse_lanes)
    tag_own[...] = jnp.concatenate([top, low, spare], axis=0).astype(jnp.bfloat16)

    def tag_copy(side):
        dy, dx = AROUND[side]
        return around.copy(tag_own, tag_wide.at[side], tag_send.at[side], tag_recv.at[side], dy, dx)

    for side, (dy, dx) in enumerate(AROUND):
        around.when_there(-dy, lambda side=side: tag_copy(side).start())

    fetch.wait()
    fetches[3].wait()
    fetches[4].wait()
    normed = normalize(tokens[...], fine_gain[...])
    arranged = pick(index_ref[: fine.quads * ROWS, 0:1], normed)
    own[...] = arranged
    halo.start()
    for q in range(fine.quads):
        spot = fine.spot(*divmod(q, fine.across))
        wide[pl.ds(spot * ROWS, ROWS), :] = arranged[q * ROWS : (q + 1) * ROWS]

    for other in fetches[5:]:
        other.wait()
    parts = split_table((fine_table, coarse_table), padded)
    fine_bias[...] = jnp.zeros_like(fine_bias)
    coarse_bias[...] = jnp.zeros_like(coarse_bias)
    chunk = 4 * QUAD // 6
    for first in range(0, 4 * QUAD, chunk):
        fill_bias(parts, number_ref, (fine_bias, coarse_bias), first, first + chunk)
        if first:
            gather.step()

    for side, (dy, dx) in enumerate(AROUND):
        around.when_there(dy, lambda side=side: tag_copy(side).wait_recv())
    tags = [tag_wide[side].astype(jnp.float32) for side in range(len(AROUND))] + [tag_own[...].astype(jnp.float32)]
    fill_masks(fine, tags, 0, fine_masks)
    fill_masks(coarse, tags, fine.quads, coarse_masks)

    gather.ready(0)
    half = width // lvls
    for lvl in range(lvls):
        part = jnp.dot(turned(own, slice(None), block_of, lons), flat(f0[lvl, 0]), preferred_element_type=jnp.float32)
        query[:, lvl * half : (lvl + 1) * half] = (part * scale).astype(jnp.bfloat16)
    halo.finish()
    for member, target in ((1, keys), (2, values)):
        gather.ready(member)

        @pl.loop(0, fine.windows // fine.columns)
        def _(band):
            count = fine.columns * WINDOW
            rows = pl.ds(pl.multiple_of(band * count, count), count)
            x = turned(wide, rows, block_of, lons)
            for lvl in range(lvls):
                part = jnp.dot(x, flat(f0[lvl, member]), preferred_element_type=jnp.float32)
                target[rows, lvl * half : (lvl + 1) * half] = part.astype(jnp.bfloat16)

    per_row = fine.across
    for first in range(0, fine.quads, per_row):
        @pl.loop(first, first + per_row, step=2)
        def _(q):
            attend(
                fine, [(q + i, group) for i in range(2) for group in range(width // LANES)], query, keys, values,
                fine_bias, fine_masks, mixed, size,
            )
        gather.step()

    own_mixed = pick(index_ref[: fine.own, 1:2], mixed[...])
    gather.ready(3)
    update = None
    for lvl in range(lvls):
        term = lax.dot_general(
            own_mixed[:, lvl * half : (lvl + 1) * half], flat(f1[lvl, 0]), NT, preferred_element_type=jnp.float32
        )
        update = term if update is None else update + term

    def put_fine(cols, value):
        fine_value[:, cols] = (tokens[:, cols].astype(jnp.float32) + value).astype(jnp.bfloat16)

    turn_back(update, block_of, lons, put_fine)
    publish = pltpu.make_async_copy(fine_value, fine_ref, local.at[1])
    publish.start()

    count = coarse.quads * ROWS
    stacked = pick(index_ref[: 4 * count, 2:3], fine_value[...]).astype(jnp.float32)
    members = [stacked[m * count : (m + 1) * count] for m in range(4)]
    mean = sum(jnp.sum(m, axis=-1, keepdims=True) for m in members) / (4 * width)
    centers = [m - mean for m in members]
    spread = sum(jnp.sum(c * c, axis=-1, keepdims=True) for c in centers) / (4 * width)
    factor = lax.rsqrt(spread + EPSILON)
    normed = jnp.concatenate(
        [(centers[m] * factor * merge_gain[:, m * width : (m + 1) * width]).astype(jnp.bfloat16) for m in range(4)],
        axis=1,
    )
    merged = None
    share = 4 * width // lvls
    for u in [u for u in range(len(units)) if units[u][0] == 2]:
        gather.ready(u)
        _, _, _, col, cols = units[u]
        for lvl in range(lvls):
            start = lvl * share + col
            term = lax.dot_general(
                normed[:, start : start + cols], flat(f2[lvl, 0, :, :, col : col + cols]), NT,
                preferred_element_type=jnp.float32,
            )
            merged = term if merged is None else merged + term

    def put_coarse(cols, value):
        two_in[:, cols] = value.astype(jnp.bfloat16)

    turn_back(merged, block_of, lons, put_coarse)
    two_own[...] = normalize(two_in[...], coarse_gain[...])
    halo_two.start()
    for q in range(coarse.quads):
        spot = coarse.spot(*divmod(q, coarse.across))
        two_wide[pl.ds(spot * ROWS, ROWS), :] = two_own[q * ROWS : (q + 1) * ROWS, :]
    gather.step(2)
    halo_two.finish()

    share = wide_two // lvls
    inner = [u for u in range(len(units)) if units[u][0] == 3]
    for u in inner:
        gather.ready(u)
        _, _, _, col, cols = units[u]
        for lvl in range(lvls):
            start = lvl * share + col
            part = jnp.dot(
                turned(two_own, slice(None), block_of, lons), flat(f3[lvl, 0, :, :, col : col + cols]),
                preferred_element_type=jnp.float32,
            )
            two_query[:, start : start + cols] = (part * scale).astype(jnp.bfloat16)
            weight = jnp.concatenate([flat(f3[lvl, k, :, :, col : col + cols]) for k in (1, 2)], axis=1)
            part = jnp.dot(
                turned(two_wide, slice(None), block_of, lons), weight, preferred_element_type=jnp.float32
            ).astype(jnp.bfloat16)
            two_keys[:, start : start + cols] = part[:, :cols]
            two_values[:, start : start + cols] = part[:, cols:]

        attend(
            coarse, [(q, (lvl * share + col) // LANES) for q in range(coarse.quads) for lvl in range(lvls)],
            two_query, two_keys, two_values, coarse_bias, coarse_masks, two_mixed, size,
        )

    update = None
    for u in [u for u in range(len(units)) if units[u][0] == 4]:
        gather.ready(u)
        _, _, _, col, cols = units[u]
        for lvl in range(lvls):
            start = lvl * share + col
            term = lax.dot_general(
                two_mixed[:, start : start + cols], flat(f4[lvl, 0, :, :, col : col + cols]), NT,
                preferred_element_type=jnp.float32,
            )
            update = term if update is None else update + term

    def put_out(cols, value):
        two_value[:, cols] = (two_in[:, cols].astype(jnp.float32) + value).astype(jnp.bfloat16)

    turn_back(update, block_of, lons, put_out)
    pitch = up_to(coarse.lon_len, 16)
    result = pick(index_ref[: coarse.lat_len * pitch, 3:4], two_value[...])
    for r in range(coarse.lat_len):
        coarse_ref[r] = result[r * pitch : r * pitch + coarse.lon_len]

    publish.wait()
    gather.end()
    for side, (dy, dx) in enumerate(AROUND):
        around.when_there(-dy, lambda side=side: tag_copy(side).wait_send())
    halo.drain()
    halo_two.drain()


def publish_kernel(fine_in, coarse_in, fine_out, coarse_out, fine_held, coarse_held, sems):
    steps = ((fine_in, fine_held, fine_out), (coarse_in, coarse_held, coarse_out))
    come = [pltpu.make_async_copy(a, b, sems.at[n]) for n, (a, b, _) in enumerate(steps)]
    leave = [pltpu.make_async_copy(b, c, sems.at[2 + n]) for n, (_, b, c) in enumerate(steps)]
    for copy in come:
        copy.start()
    for n in range(2):
        come[n].wait()
        leave[n].start()
    for copy in leave:
        copy.wait()


def level_scratch(plan, features, heads):
    rows, all_rows = plan.quads * ROWS, plan.windows * WINDOW
    return [
        pltpu.VMEM((rows, features), jnp.bfloat16),
        pltpu.VMEM((all_rows, features), jnp.bfloat16),
        pltpu.VMEM((rows, features), jnp.bfloat16),
        pltpu.VMEM((all_rows, features), jnp.bfloat16),
        pltpu.VMEM((all_rows, features), jnp.bfloat16),
        pltpu.VMEM((rows, features), jnp.bfloat16),
        pltpu.VMEM((heads, WINDOW, LANES), jnp.float32),
        pltpu.VMEM((plan.quads, ROWS, LANES), jnp.float32),
    ]


def shards(
    tokens, fine_tags, coarse_tags, fine_gain, fine_inward, fine_outward, fine_table, merge_gain,
    merge_weight, coarse_gain, coarse_inward, coarse_outward, coarse_table,
):
    _, lat_len, lon_len, width = tokens.shape
    fine, coarse = Plan(lat_len, lon_len), Plan(lat_len // 2, lon_len // 2)
    weights = [fine_inward, fine_outward[None], merge_weight[None], coarse_inward, coarse_outward[None]]
    grps, lats, lons, lvls = (lax.axis_size(a) for a in ("grp", "lat", "lon", "lvl"))
    split = grps == 2 and lats == 2 and all(w.shape[1] % LANES == 0 for w in weights)
    units = weight_units(weights)
    wide_two = coarse_inward.shape[1] * lons
    heads, heads_two = fine_table.shape[0], coarse_table.shape[0]
    pitch = up_to(coarse.lon_len, 16)

    columns = [fine.natural(), fine.back(fine.lon_len), patches(fine, coarse), coarse.back(pitch)]
    index = np.full((max(len(c) for c in columns), len(columns)), -1, np.int32)
    for n, column in enumerate(columns):
        index[: len(column), n] = column
    lane = np.concatenate([np.stack(p.lanes()) for p in (fine, coarse)], axis=1).astype(np.int32)

    small = [
        fine_tags.reshape(lat_len, 1, lon_len), coarse_tags.reshape(coarse.lat_len, 1, coarse.lon_len), lane,
        fine_gain[None], index, fine_table, coarse_table, offset_numbers(), merge_gain[None], coarse_gain[None],
    ]
    dma = pltpu.SemaphoreType.DMA
    bf16 = jnp.bfloat16
    sides, tag_count = len(AROUND), up_to(fine.quads + coarse.quads, 16)
    fine_out, coarse_out = pl.pallas_call(
        functools.partial(kernel, fine, coarse, units, split),
        out_shape=[
            jax.ShapeDtypeStruct((fine.own, width), bf16),
            jax.ShapeDtypeStruct((coarse.lat_len, coarse.lon_len, wide_two), bf16),
        ],
        in_specs=[HBM] * (1 + SMALL + len(weights)),
        out_specs=[ANY, VMEM],
        scratch_shapes=[pltpu.VMEM(x.shape, x.dtype) for x in small]
        + [pltpu.VMEM((fine.own, width), bf16)]
        + level_scratch(fine, width, heads)
        + [pltpu.VMEM((fine.own, width), bf16)]
        + level_scratch(coarse, wide_two, heads_two)
        + [pltpu.VMEM((coarse.quads * ROWS, wide_two), bf16)] * 2
        + [
            pltpu.VMEM((heads + heads_two, up_to(fine_table.shape[1], LANES)), jnp.float32),
            pltpu.VMEM((tag_count, LANES), bf16),
            pltpu.VMEM((sides, tag_count, LANES), bf16),
        ]
        + [pltpu.VMEM((lvls, w.shape[0], lons, w.shape[1], w.shape[2]), bf16) for w in weights]
        + [dma((2 + SMALL,)), dma((sides,)), dma((sides,))]
        + [dma((len(fine.halo),))] * 2
        + [dma((len(coarse.halo),))] * 2
        + gather_scratch(units),
        compiler_params=pltpu.CompilerParams(collective_id=1, has_side_effects=True, vmem_limit_bytes=LIMIT),
        name="levels",
    )(
        tokens.reshape(fine.own, width), *small, *weights,
    )
    fine_out, coarse_out = pl.pallas_call(
        publish_kernel,
        out_shape=[jax.ShapeDtypeStruct(x.shape, x.dtype) for x in (fine_out, coarse_out)],
        in_specs=[HBM] * 2,
        out_specs=[HBM] * 2,
        scratch_shapes=[pltpu.VMEM(x.shape, x.dtype) for x in (fine_out, coarse_out)] + [dma((4,))],
        name="publish",
    )(fine_out, coarse_out)
    return fine_out.reshape(tokens.shape), coarse_out[None]


def solution(mesh):
    placed = (
        P(("grp", "lvl"), "lat", "lon", None),
        P(("grp", "lvl"), "lat", "lon"),
        P(("grp", "lvl"), "lat", "lon"),
        P(),
        P(None, "lon", "lvl"),
        P("lon", "lvl"),
        P(),
        P(),
        P("lon", "lvl"),
        P(),
        P(None, "lon", "lvl"),
        P("lon", "lvl"),
        P(),
    )
    return jax.shard_map(
        shards,
        mesh=mesh,
        in_specs=placed,
        out_specs=(P(("grp", "lvl"), "lat", "lon", None), P(("grp", "lvl"), "lat", "lon", None)),
        check_vma=False,
    )
```
